512 devices in a mesh: tm: 256 (over x, z, y), det: 2 (over core).
Axes of the slice: x: 4, y: 8, z: 8, core: 2. Of those that a mesh axis runs over, the one named last changes fastest.
Arguments:
- strain: float32 [2, 1024, 192, 512], P('det', 'tm'), may hold values from -24 to 24
- final_half: float32 [2, 192, 512], P('det'), may hold values from -6 to 6
- intersection_function: float32 [16384], P('det'), may hold values from -1 to 1
- notch_mask: int32 [16384], P('det'), may hold values 0 or 1
- quality_flags: int32 [1024], P('tm'), may hold values 0 or 1
Outputs:
- csd: float32 [1024, 2, 16384], P('tm', None, 'det')
- stats: float32 [3, 1024], P(None, 'tm')
- combined: float32 [2], replicated
The draws below stay inside these ranges and needn't reach their ends.
All inputs are finite; a program needn't handle non-finite values. No bound on the sum of `notch_mask` or of `quality_flags` on one device may be relied on, other than what follows from the above.
Results may differ from the reference program's by a relative error of at most 0.0003.
Values sent between devices are 32-bit elements; how exact they have to be, the bound alone decides.
A program may use at most 64 MiB of HBM per device.

```python
import jax
import jax.numpy as jnp
from jax import lax

N2 = 512
K2 = 256
BIN = 6
SEGMENTS = 1024
HALF_ROWS = 192
KC = 16384


def draw_strain(key, part):
    base_key = jax.random.fold_in(key, 11)
    noise_key, level_key = jax.random.split(base_key, 2)
    shape = (2, SEGMENTS, HALF_ROWS, N2)
    position = jnp.arange(SEGMENTS, dtype=jnp.float32) / SEGMENTS
    rough = jnp.exp(jax.random.uniform(level_key, (2, SEGMENTS), jnp.float32, jnp.log(0.7), jnp.log(1.4)))
    noise = jnp.clip(jax.random.normal(noise_key, shape, jnp.float32), -6.0, 6.0)
    trend = 3.0 ** (0.5 * position)
    values = noise * (trend[None, :] * rough)[:, :, None, None]
    return values.astype(jnp.float32)


def plant(result, key, least, high):
    index_at = [jax.random.randint(jax.random.fold_in(key, axis), (), 0, length) for axis, length in enumerate(result.shape)]
    widest = result.shape.index(max(result.shape))
    next_to = index_at[:widest] + [(index_at[widest] + 1) % result.shape[widest]] + index_at[widest + 1:]
    return result.at[tuple(index_at)].set(least).at[tuple(next_to)].set(high)


def steps_of(rng, dims, shards, least, top_value):
    def one(dim, blocks):
        draws = jax.random.uniform(jax.random.fold_in(jax.random.fold_in(rng, 6), dim), (blocks,), jnp.float32, least / len(shards), top_value / len(shards))
        return jnp.repeat(jnp.exp(draws), dims[dim] // blocks).reshape((-1,) + (1,) * (len(dims) - dim - 1))

    factor_of = one(*shards[0])
    for cut in shards[1:]:
        factor_of = factor_of * one(*cut)
    return factor_of


def gaussian(stream_key, extent, deviation, bound, cuts=(), held_as=jnp.bfloat16):
    array = jax.random.normal(stream_key, extent, jnp.float32) * deviation
    if len(cuts) > 0:
        array = steps_of(stream_key, extent, cuts, -0.22, 0.18) * array
    return jnp.clip(array, min=-bound, max=bound).astype(held_as)


def setup_inputs(seed: int = 0) -> dict:
    arg_keys = jax.random.split(jax.random.key(seed), 6)
    return {
        "strain": draw_strain(jax.random.fold_in(arg_keys[5], 71), 0),
        "final_half": gaussian(arg_keys[1], (2, HALF_ROWS, N2), 1.5, 6.0, ((0, 2),), jnp.float32),
        "intersection_function": jnp.clip(jax.random.uniform(arg_keys[2], (KC,), jnp.float32, -1.0, 1.0) * steps_of(arg_keys[2], (KC,), ((0, 2),), -0.4, 0.0), -1.0, 1.0),
        "notch_mask": plant((jax.random.randint(arg_keys[3], (KC,), 0, 8) < 7).astype(jnp.int32), jax.random.fold_in(arg_keys[3], 1), 0, 1),
        "quality_flags": plant((jax.random.randint(arg_keys[4], (SEGMENTS,), 0, 8) < 7).astype(jnp.int32), jax.random.fold_in(arg_keys[4], 1), 0, 1),
    }


INTERSECTION_CORR = 27.0 / 154.0

def reference(strain, final_half, intersection_function, notch_mask, quality_flags):
    segments = strain.shape[1]
    half_rows = strain.shape[2]
    columns = strain.shape[3]
    length = 2 * half_rows * columns
    fine_count = 2 * half_rows * K2
    sample_index = jnp.arange(length, dtype=jnp.int32).astype(jnp.float32)
    window = jnp.sin(jnp.pi * sample_index / length) ** 2
    scale_factor = (8.0 / (3.0 * length)) ** 0.5

    def spectra(segment_at):
        upper_half = lax.dynamic_index_in_dim(strain, segment_at, 1, keepdims=False)
        next_half = lax.dynamic_index_in_dim(strain, jnp.minimum(segment_at + 1, segments - 1).astype(jnp.int32), 1, keepdims=False)
        lower_half = jnp.where(segment_at + 1 < segments, next_half, final_half)
        windowed = jnp.concatenate([upper_half, lower_half], axis=1).reshape(2, length) * window
        fine_bins = jnp.fft.fft(windowed, axis=1)[:, :fine_count]
        part_real = fine_bins.real * scale_factor
        part_imag = fine_bins.imag * scale_factor
        cross_real = part_real[0] * part_real[1] + part_imag[0] * part_imag[1]
        cross_imag = part_real[0] * part_imag[1] - part_imag[0] * part_real[1]
        power = part_real * part_real + part_imag * part_imag
        cross_coarse = jnp.stack([cross_real, cross_imag]).reshape(2, fine_count // BIN, BIN).sum(axis=-1) / BIN
        power_coarse = power.reshape(2, fine_count // BIN, BIN).sum(axis=-1) / BIN
        return (cross_coarse, power_coarse)
    cross_coarse, power_coarse = lax.map(spectra, jnp.arange(segments, dtype=jnp.int32))
    coarse_bins = fine_count // BIN
    zero_row = jnp.zeros_like(power_coarse[:1])
    left_power = jnp.concatenate([zero_row, power_coarse[:-1]], axis=0)
    right_power = jnp.concatenate([power_coarse[1:], zero_row], axis=0)
    positions = jnp.arange(segments, dtype=jnp.int32)
    has_left = (positions > 0).astype(jnp.float32)[:, None, None]
    has_right = (positions < segments - 1).astype(jnp.float32)[:, None, None]
    mean_power = (has_left * left_power + has_right * right_power) / (has_left + has_right)
    filter_weight = notch_mask.astype(jnp.float32) * intersection_function / (mean_power[:, 0] * mean_power[:, 1])
    numerator = lax.optimization_barrier(jnp.sum(filter_weight * cross_coarse[:, 0], axis=-1))
    denominator = lax.optimization_barrier(jnp.sum(filter_weight * intersection_function, axis=-1))
    estimate = jnp.sqrt(12.0 * coarse_bins) * numerator / denominator
    spread = jnp.sqrt(coarse_bins / denominator)
    quality = quality_flags.astype(jnp.float32)
    tail_zero = jnp.zeros((1,), jnp.float32)
    up_next = jnp.concatenate([quality[1:] * spread[1:], tail_zero])
    down_next = jnp.concatenate([quality[1:] / spread[1:], tail_zero])
    covariance = INTERSECTION_CORR * quality * spread * up_next
    pair_term = INTERSECTION_CORR * quality / spread * down_next
    weight = quality / (spread * spread)
    weight_sum = jnp.sum(weight)
    weighted_sum = jnp.sum(weight * estimate)
    pair_sum = jnp.sum(pair_term)
    scale_root = jnp.sqrt(jnp.float32(segments))
    combined = scale_root * jnp.stack([weighted_sum / weight_sum, jnp.sqrt(weight_sum + 2.0 * pair_sum) / weight_sum])
    stats = jnp.stack([estimate, spread, covariance])
    return (cross_coarse, stats, combined)
```

```python
import functools

import jax
import jax.numpy as jnp
import numpy as np
from jax import lax
from jax.experimental import pallas as pl
from jax.experimental.pallas import tpu as pltpu
from jax.sharding import PartitionSpec as P

MESH = pl.DeviceIdType.MESH
F32 = jnp.float32
BF16 = jnp.bfloat16

HALF = 192
FULL = 384
COLS = 512
LENGTH = FULL * COLS
KBLK = 256
BIN = 6
GROUPS = FULL // BIN
COARSE = 16384
KPAD = 256
CORR = 27.0 / 154.0
SEG = 4


def split_np(table):
    high = table.astype(np.float32).astype(BF16)
    low = (table - high.astype(np.float64)).astype(np.float32).astype(BF16)
    return high, low


@functools.cache
def tables():
    row = np.arange(HALF)
    col = np.arange(COLS)
    window = np.sin(np.pi * (row[:, None] * COLS + col[None, :]) / LENGTH) ** 2

    ones, twists = [], []
    for parity in range(2):
        bins = np.concatenate([BIN * np.arange(GROUPS) + r for r in range(parity, BIN, 2)])
        angle = 2.0 * np.pi * (bins[:, None] * row[None, :] % FULL) / FULL
        one = np.concatenate([np.cos(angle), -np.sin(angle)], axis=0)
        ones.append(np.pad(one, ((0, 0), (0, KPAD - HALF))))
        turn = 2.0 * np.pi * (bins[:, None] * col[None, :] % LENGTH) / LENGTH
        twists.append(np.stack([np.cos(turn), np.sin(turn)]))
    one_hi, one_lo = split_np(np.stack(ones))

    twos = []
    for q in range(2):
        parts = []
        for band in range(2):
            k2 = 2 * (64 * band + np.arange(64)) + q
            angle = 2.0 * np.pi * (np.arange(256)[:, None] * k2[None, :] % COLS) / COLS
            c, s = np.cos(angle), np.sin(angle)
            parts.append(np.concatenate([c, s], axis=0))
            parts.append(np.concatenate([-s, c], axis=0))
        twos.append(np.concatenate(parts, axis=1))
    two_hi, two_lo = split_np(np.stack(twos) * (8.0 / (3.0 * LENGTH) / BIN) ** 0.5)
    return (
        window.astype(np.float32),
        np.stack([one_hi, one_lo], axis=1),
        np.stack(twists).astype(np.float32),
        np.stack([two_hi, two_lo], axis=1),
    )


def kernel(
    dims,
    strain, final, func, mask, flags, window, ones, twist, twos,
    csd, stats, combined,
    h, win, one, twi, two, fnat, mnat, rhs, y, lhs, xb, rb, pw, pn, pp, ob, sums, rsums, gath, flag, rflag, fg, re_c,
    load_sem, half_send, half_recv, x_send, x_recv, p_send, p_recv, s_sem, g_send, g_recv, o_sem,
):
    nx, nz, ny = dims
    total = nx * nz * ny
    me = lax.axis_index("tm")
    det = lax.axis_index("det")
    cy = lax.rem(me, ny)
    cz = lax.rem(me // ny, nz)
    cx = me // (ny * nz)
    prev = lax.rem(me + total - 1, total)
    following = lax.rem(me + 1, total)
    first = me == 0
    last = me == total - 1

    def y_peer(k):
        return (cx * nz + cz) * ny + k

    def z_peer(k):
        return (cx * nz + k) * ny + cy

    def x_peer(k):
        return (k * nz + cz) * ny + cy

    axes = ((ny, cy, y_peer), (nz, cz, z_peer), (nx, cx, x_peer))

    barrier = pltpu.get_barrier_semaphore()
    peers = [(prev, det), (following, det), (me, 1 - det)]
    for count, mine, peer in axes:
        for d in range(1, count):
            peers.append((peer(lax.rem(mine + d, count)), det))
    for peer in peers:
        pl.semaphore_signal(barrier, inc=1, device_id=peer, device_id_type=MESH)

    loads = []

    def load(src, dst):
        copy = pltpu.make_async_copy(src, dst, load_sem.at[len(loads)])
        copy.start()
        loads.append(copy)

    load(window, win)
    for s in range(SEG):
        load(strain.at[0, s], h.at[s])
    for parity in range(2):
        for part in range(3):
            load(ones.at[parity, part % 2], one.at[parity, :, pl.ds(KPAD * part, KPAD)])
    load(twist, twi)
    for q in range(2):
        for part in range(3):
            load(twos.at[q, (0, 0, 1)[part]], two.at[q, pl.ds(512 * part, 512)])
    load(func, fnat)
    load(mask, mnat)

    flag[...] = jnp.full((8, 128), flags[0].astype(F32), F32)
    gap = jnp.zeros((KPAD - HALF, COLS), BF16)
    for parity in range(2):
        for part in range(3):
            rhs[parity, pl.ds(KPAD * part + HALF, KPAD - HALF), :] = gap
    sums[...] = jnp.zeros((16, 128), F32)

    pl.semaphore_wait(barrier, len(peers))

    def half_copy(p):
        cols = pl.ds(256 * p, 256)
        return pltpu.make_async_remote_copy(
            src_ref=strain.at[0, 0, :, cols],
            dst_ref=h.at[SEG, :, cols],
            send_sem=half_send.at[p],
            recv_sem=half_recv.at[p],
            device_id=(prev, det),
            device_id_type=MESH,
        )

    @pl.when(jnp.logical_not(first))
    def _():
        for p in range(2):
            half_copy(p).start()

    def flag_copy():
        return pltpu.make_async_remote_copy(
            src_ref=flag, dst_ref=rflag, send_sem=p_send.at[3], recv_sem=p_recv.at[3],
            device_id=(prev, det), device_id_type=MESH,
        )

    flag_copy().start()

    def last_copy():
        return pltpu.make_async_copy(final.at[0], h.at[SEG], o_sem.at[SEG])

    @pl.when(last)
    def _():
        last_copy().start()

    for copy in loads:
        copy.wait()

    low_lane = lax.broadcasted_iota(jnp.int32, (64, 128), 1) < 64

    f_nat = fnat[...]
    g_nat = f_nat * mnat[...].astype(F32)
    fg[...] = jnp.concatenate(
        [
            jnp.where(low_lane, f_nat, pltpu.roll(g_nat, 64, 1)),
            jnp.where(low_lane, pltpu.roll(f_nat, 64, 1), g_nat),
        ],
        axis=0,
    ).T

    def split(value):
        high = value.astype(BF16)
        return high, (value - high.astype(F32)).astype(BF16)

    def transform(s, arriving):
        for p in range(2):
            cols = pl.ds(256 * p, 256)
            if arriving:

                @pl.when(jnp.logical_not(last))
                def _():
                    half_copy(p).wait_recv()

                if p == 0:

                    @pl.when(last)
                    def _():
                        last_copy().wait()

            def windowed(i, carry):
                rows = pl.ds(pl.multiple_of(16 * i, 16), 16)
                upper = h[s, rows, cols]
                lower = h[s + 1, rows, cols]
                w = win[rows, cols]
                for parity, value in ((0, lower + w * (upper - lower)), (1, w * (upper + lower) - lower)):
                    high, low = split(value)
                    rhs[parity, rows, cols] = high
                    rhs[parity, pl.ds(pl.multiple_of(KPAD + 16 * i, 16), 16), cols] = high
                    rhs[parity, pl.ds(pl.multiple_of(2 * KPAD + 16 * i, 16), 16), cols] = low
                return carry

            lax.fori_loop(0, HALF // 16, windowed, 0)
            for parity in range(2):
                y[parity, :, cols] = jnp.dot(one[parity], rhs[parity, :, cols], preferred_element_type=F32)

        def turned(i, carry):
            rows = pl.ds(pl.multiple_of(16 * i, 16), 16)
            for parity in range(2):
                real = y[parity, rows, :]
                imag = y[parity, pl.ds(pl.multiple_of(HALF + 16 * i, 16), 16), :]
                c = twi[parity, 0, rows, :]
                n = twi[parity, 1, rows, :]
                zr = real * c + imag * n
                zi = imag * c - real * n
                out_rows = pl.ds(pl.multiple_of(HALF * parity + 16 * i, 16), 16)
                for q in range(2):
                    for at, z in ((0, zr), (256, zi)):
                        high, low = split(z[:, :256] + z[:, 256:] if q == 0 else z[:, :256] - z[:, 256:])
                        lhs[q, out_rows, pl.ds(at, 256)] = high
                        lhs[q, out_rows, pl.ds(512 + at, 256)] = low
                        lhs[q, out_rows, pl.ds(1024 + at, 256)] = high
            return carry

        lax.fori_loop(0, HALF // 16, turned, 0)
        for q in range(2):
            out = jnp.dot(lhs[q], two[q], preferred_element_type=F32)
            xb[s, q, 0] = out[:, :128]
            xb[s, q, 1] = out[:, 128:]
            x_copy(s, q).start()

    def x_copy(s, q):
        return pltpu.make_async_remote_copy(
            src_ref=xb.at[s, q, 1 - det], dst_ref=rb.at[s, q], send_sem=x_send.at[s, q], recv_sem=x_recv.at[s, q],
            device_id=(me, 1 - det), device_id_type=MESH,
        )

    sign = 1.0 - 2.0 * det.astype(F32)

    def crossed(s):
        parts = []
        for q in range(2):
            x_copy(s, q).wait_recv()
            same = jnp.zeros((64, 128), F32)
            swap = jnp.zeros((64, 128), F32)
            power_a = jnp.zeros((64, 128), F32)
            power_b = jnp.zeros((64, 128), F32)
            for r in range(BIN):
                rows = pl.ds(64 * r, 64)
                a = xb[s, q, det, rows, :]
                b = rb[s, q, rows, :]
                same = same + a * b
                swap = swap + a * pltpu.roll(b, 64, 1)
                power_a = power_a + a * a
                power_b = power_b + b * b
            parts.append(
                (
                    same + pltpu.roll(same, 64, 1),
                    swap - pltpu.roll(swap, 64, 1),
                    power_a + pltpu.roll(power_a, 64, 1),
                    power_b + pltpu.roll(power_b, 64, 1),
                )
            )
        even, odd = parts
        real = jnp.where(low_lane, even[0], odd[0])
        imag = jnp.where(low_lane, even[1], -odd[1]) * sign
        pw[s, 0] = jnp.where(low_lane, even[2], odd[2])
        pw[s, 1] = jnp.where(low_lane, even[3], odd[3])
        re_c[s] = real
        turned = jnp.concatenate([real, imag], axis=0).T
        top, bottom = turned[:64], turned[64:]
        ob[s, pl.ds(0, 64, stride=2), :] = jnp.where(low_lane, top, pltpu.roll(bottom, 64, 1))
        ob[s, pl.ds(1, 64, stride=2), :] = jnp.where(low_lane, pltpu.roll(top, 64, 1), bottom)
        out_copy(s).start()

    def out_copy(s):
        return pltpu.make_async_copy(ob.at[s], csd.at[s], o_sem.at[s])

    def power_copy(which):
        if which < 2:
            return pltpu.make_async_remote_copy(
                src_ref=pw.at[which], dst_ref=pn.at[which], send_sem=p_send.at[which], recv_sem=p_recv.at[which],
                device_id=(prev, det), device_id_type=MESH,
            )
        return pltpu.make_async_remote_copy(
            src_ref=pw.at[SEG - 1], dst_ref=pp, send_sem=p_send.at[2], recv_sem=p_recv.at[2],
            device_id=(following, det), device_id_type=MESH,
        )

    transform(0, False)
    transform(1, False)
    crossed(0)
    power_copy(0).start()
    transform(2, False)
    crossed(1)
    power_copy(1).start()
    crossed(2)
    transform(3, True)
    crossed(3)
    power_copy(2).start()

    f_t = fg[pl.ds(0, 64), :]
    g_t = fg[pl.ds(64, 64), :]

    def accumulate(s, left, right, weight_left, weight_right):
        mean_a = left(0) * weight_left + right(0) * weight_right
        mean_b = left(1) * weight_left + right(1) * weight_right
        filt = g_t / (mean_a * mean_b)
        if s < SEG:
            sums[pl.ds(s, 1), :] = jnp.sum(filt * re_c[s], axis=0, keepdims=True)
        sums[pl.ds(8 + s, 1), :] = jnp.sum(filt * f_t, axis=0, keepdims=True)

    def own(s):
        return lambda a: pw[s, a]

    def ahead(s):
        return lambda a: pn[s, a]

    for s in (1, 2):
        accumulate(s, own(s - 1), own(s + 1), 0.5, 0.5)
    power_copy(0).wait_recv()
    ends = jnp.where(last, 1.0, 0.5).astype(F32)
    accumulate(3, own(2), ahead(0), ends, 1.0 - ends)
    power_copy(1).wait_recv()
    accumulate(4, own(3), ahead(1), 0.5, 0.5)
    power_copy(2).wait_recv()
    starts = jnp.where(first, 1.0, 0.5).astype(F32)
    accumulate(0, lambda a: pp[a], own(1), 1.0 - starts, starts)

    sum_copy = pltpu.make_async_remote_copy(
        src_ref=sums, dst_ref=rsums, send_sem=s_sem.at[0], recv_sem=s_sem.at[1],
        device_id=(me, 1 - det), device_id_type=MESH,
    )
    sum_copy.start()
    flag_copy().wait_recv()
    lane = lax.broadcasted_iota(jnp.int32, (8, 128), 1)
    row = lax.broadcasted_iota(jnp.int32, (8, 128), 0)
    quality = jnp.zeros((8, 128), F32)
    for s in range(SEG):
        quality = jnp.where(lane == s, flags[s].astype(F32), quality)
    quality = jnp.where(lane == SEG, rflag[...], quality)
    sum_copy.wait_recv()
    whole = jnp.sum(sums[...] + rsums[...], axis=1, keepdims=True)

    def to_lanes(column):
        spread_out = jnp.where(lane == row, jnp.broadcast_to(column, (8, 128)), 0.0)
        return jnp.broadcast_to(jnp.sum(spread_out, axis=0, keepdims=True), (8, 128))

    numerator = to_lanes(whole[:8])
    denominator = to_lanes(whole[8:])
    spread = jnp.sqrt(float(COARSE) / denominator)
    estimate = float(np.sqrt(12.0 * COARSE)) * numerator / denominator
    next_spread = pltpu.roll(spread, 127, 1)
    next_quality = pltpu.roll(quality, 127, 1)
    no_next = jnp.logical_and(lane == SEG - 1, last)
    up_next = jnp.where(no_next, 0.0, next_quality * next_spread)
    down_next = jnp.where(no_next, 0.0, next_quality / next_spread)
    covariance = CORR * quality * spread * up_next
    pair_term = CORR * quality / spread * down_next
    weight = quality / (spread * spread)
    rows3 = jnp.where(row == 0, estimate, jnp.where(row == 1, spread, covariance))
    stats[...] = rows3[:3, :SEG]
    terms = jnp.where(row == 0, weight, jnp.where(row == 1, weight * estimate, pair_term))
    terms = jnp.where(jnp.logical_and(lane < SEG, row < 3), terms, 0.0)

    for axis, (count, mine, peer) in enumerate(axes):
        gath[axis, mine] = terms

        def gather_copy(d, axis=axis, count=count, mine=mine, peer=peer):
            return pltpu.make_async_remote_copy(
                src_ref=gath.at[axis, mine], dst_ref=gath.at[axis, mine],
                send_sem=g_send.at[axis, d], recv_sem=g_recv.at[axis, mine],
                device_id=(peer(lax.rem(mine + d, count)), det), device_id_type=MESH,
            )

        for d in range(1, count):
            gather_copy(d).start()
        for d in range(1, count):
            source = lax.rem(mine + d, count)
            pltpu.make_async_remote_copy(
                src_ref=gath.at[axis, source], dst_ref=gath.at[axis, source],
                send_sem=g_send.at[axis, d], recv_sem=g_recv.at[axis, source],
                device_id=(peer(source), det), device_id_type=MESH,
            ).wait_recv()
        terms = gath[axis, 0]
        for k in range(1, count):
            terms = terms + gath[axis, k]

    sweep = jnp.sum(terms, axis=1, keepdims=True)
    weight_sum, weighted_sum, pair_sum = sweep[0:1], sweep[1:2], sweep[2:3]
    root = float(np.sqrt(SEG * total))
    pick = lax.broadcasted_iota(jnp.int32, (1, 2), 1)
    combined[...] = jnp.where(
        pick == 0, root * (weighted_sum / weight_sum), root * (jnp.sqrt(weight_sum + 2.0 * pair_sum) / weight_sum)
    )

    for axis, (count, mine, peer) in enumerate(axes):
        for d in range(1, count):
            pltpu.make_async_remote_copy(
                src_ref=gath.at[axis, mine], dst_ref=gath.at[axis, mine],
                send_sem=g_send.at[axis, d], recv_sem=g_recv.at[axis, mine],
                device_id=(peer(lax.rem(mine + d, count)), det), device_id_type=MESH,
            ).wait_send()

    @pl.when(jnp.logical_not(first))
    def _():
        for p in range(2):
            half_copy(p).wait_send()

    flag_copy().wait_send()
    for which in range(3):
        power_copy(which).wait_send()
    for s in range(SEG):
        out_copy(s).wait()
        for q in range(2):
            x_copy(s, q).wait_send()
    sum_copy.wait_send()


def on_device(dims, strain, final_half, intersection_function, notch_mask, quality_flags):
    window, ones, twist, twos = tables()
    any_space = pl.BlockSpec(memory_space=pl.ANY)
    vmem = pl.BlockSpec(memory_space=pltpu.VMEM)
    smem = pl.BlockSpec(memory_space=pltpu.SMEM)
    dma = pltpu.SemaphoreType.DMA
    csd, stats, combined = pl.pallas_call(
        functools.partial(kernel, dims),
        out_shape=(
            jax.ShapeDtypeStruct((SEG, 128, 128), F32),
            jax.ShapeDtypeStruct((3, SEG), F32),
            jax.ShapeDtypeStruct((1, 2), F32),
        ),
        in_specs=[any_space, any_space, any_space, any_space, smem, any_space, any_space, any_space, any_space],
        out_specs=(any_space, vmem, vmem),
        scratch_shapes=[
            pltpu.VMEM((SEG + 1, HALF, COLS), F32),
            pltpu.VMEM((HALF, COLS), F32),
            pltpu.VMEM((2, FULL, 3 * KPAD), BF16),
            pltpu.VMEM((2, 2, HALF, COLS), F32),
            pltpu.VMEM((2, 3 * COLS, 256), BF16),
            pltpu.VMEM((64, 128), F32),
            pltpu.VMEM((64, 128), jnp.int32),
            pltpu.VMEM((2, 3 * KPAD, COLS), BF16),
            pltpu.VMEM((2, FULL, COLS), F32),
            pltpu.VMEM((2, FULL, 3 * COLS), BF16),
            pltpu.VMEM((SEG, 2, 2, FULL, 128), F32),
            pltpu.VMEM((SEG, 2, FULL, 128), F32),
            pltpu.VMEM((SEG, 2, 64, 128), F32),
            pltpu.VMEM((2, 2, 64, 128), F32),
            pltpu.VMEM((2, 64, 128), F32),
            pltpu.VMEM((SEG, 128, 128), F32),
            pltpu.VMEM((16, 128), F32),
            pltpu.VMEM((16, 128), F32),
            pltpu.VMEM((3, 8, 8, 128), F32),
            pltpu.VMEM((8, 128), F32),
            pltpu.VMEM((8, 128), F32),
            pltpu.VMEM((128, 128), F32),
            pltpu.VMEM((SEG, 64, 128), F32),
            dma((20,)),
            dma((2,)),
            dma((2,)),
            dma((SEG, 2)),
            dma((SEG, 2)),
            dma((4,)),
            dma((4,)),
            dma((2,)),
            dma((3, 8)),
            dma((3, 8)),
            dma((SEG + 1,)),
        ],
        compiler_params=pltpu.CompilerParams(
            collective_id=0, has_side_effects=True, vmem_limit_bytes=67_043_328
        ),
    )(
        strain,
        final_half,
        intersection_function.reshape(64, 128),
        notch_mask.reshape(64, 128),
        quality_flags,
        window,
        ones,
        twist,
        twos,
    )
    csd = csd.reshape(SEG, 64, 2, 128).transpose(0, 2, 1, 3).reshape(SEG, 2, 64 * 128)
    return csd, stats, combined.reshape(2)


def solution(mesh):
    count = mesh.shape["tm"]
    dims = (4, 8, 8) if count == 256 else (2, 2, count // 4)
    return jax.shard_map(
        functools.partial(on_device, dims),
        mesh=mesh,
        in_specs=(P("det", "tm", None, None), P("det", None, None), P("det"), P("det"), P("tm")),
        out_specs=(P("tm", None, "det"), P(None, "tm"), P()),
        check_vma=False,
    )
```

```python
import functools

import jax
import jax.numpy as jnp
import numpy as np
from jax import lax
from jax.experimental import pallas as pl
from jax.experimental.pallas import tpu as pltpu
from jax.sharding import PartitionSpec as P

MESH = pl.DeviceIdType.MESH
F32 = jnp.float32
BF16 = jnp.bfloat16

HALF = 192
FULL = 384
COLS = 512
LENGTH = FULL * COLS
KBLK = 256
BIN = 6
GROUPS = FULL // BIN
COARSE = 16384
KPAD = 256
CORR = 27.0 / 154.0
SEG = 4
EVEN, ODD = 112, 96
ROWS = EVEN + ODD


def split_np(table):
    high = table.astype(np.float32).astype(BF16)
    low = (table - high.astype(np.float64)).astype(np.float32).astype(BF16)
    return high, low


@functools.cache
def tables():
    row = np.arange(HALF)
    col = np.arange(COLS)
    window = np.sin(np.pi * (row[:, None] * COLS + col[None, :]) / LENGTH) ** 2

    ones, twists = [], []
    for slabs in (((0, 48, 33), (2, 64, 64)), ((1, 64, 64), (3, 32, 32))):
        bins = np.concatenate([BIN * np.arange(rows) + r for r, rows, _ in slabs])
        keep = np.concatenate([np.arange(rows) < used for _, rows, used in slabs])[:, None]
        angle = 2.0 * np.pi * (bins[:, None] * row[None, :] % FULL) / FULL
        one = np.concatenate([np.cos(angle) * keep, -np.sin(angle) * keep], axis=0)
        ones.append(np.pad(one, ((0, 0), (0, KPAD - HALF))))
        turn = 2.0 * np.pi * (bins[:, None] * col[None, :] % LENGTH) / LENGTH
        twists.append(np.stack([np.cos(turn), np.sin(turn)]))
    one_hi, one_lo = split_np(np.concatenate(ones))

    twos = []
    t = np.arange(32)
    for q in range(4):
        parts = []
        for band in range(2):
            direct, mirrored = 32 * band + t, 127 - 32 * band - t
            k2 = 4 * np.concatenate([direct, mirrored] if q % 2 == 0 else [mirrored, direct]) + q
            angle = 2.0 * np.pi * (np.arange(128)[:, None] * k2[None, :] % COLS) / COLS
            c, s = np.cos(angle), np.sin(angle)
            parts.append(np.concatenate([c, s], axis=0))
            parts.append(np.concatenate([-s, c], axis=0))
        twos.append(np.concatenate(parts, axis=1))
    two_hi, two_lo = split_np(np.stack(twos) * (8.0 / (3.0 * LENGTH) / BIN) ** 0.5)
    return (
        window.astype(np.float32),
        np.stack([one_hi, one_lo]),
        np.concatenate(twists, axis=1).astype(np.float32),
        np.stack([two_hi, two_lo], axis=1),
    )


def kernel(
    dims,
    strain, final, func, mask, flags, window, ones, twist, twos,
    csd, stats, combined,
    h, win, one, twi, two, fnat, mnat, rhs, y, lhs, xb, rb, pw, halo, ob, sums, rsums, gath, fg, re_c,
    load_sem, half_send, half_recv, x_send, x_recv, p_sem, s_sem, g_send, g_recv, o_sem, near_sem, far_sem,
):
    nx, nz, ny = dims
    total = nx * nz * ny
    me = lax.axis_index("tm")
    det = lax.axis_index("det")
    cy = lax.rem(me, ny)
    cz = lax.rem(me // ny, nz)
    cx = me // (ny * nz)
    prev = lax.rem(me + total - 1, total)
    following = lax.rem(me + 1, total)
    first = me == 0
    last = me == total - 1

    def y_peer(k):
        return (cx * nz + cz) * ny + k

    def z_peer(k):
        return (cx * nz + k) * ny + cy

    def x_peer(k):
        return (k * nz + cz) * ny + cy

    axes = ((ny, cy, y_peer), (nz, cz, z_peer), (nx, cx, x_peer))

    barrier = pltpu.get_barrier_semaphore()
    around = [(peer(lax.rem(mine + d, count)), det) for count, mine, peer in axes for d in (1, count - 1)]
    neighbours = [(prev, det), (following, det), (me, 1 - det)] + around
    for peer in neighbours:
        pl.semaphore_signal(barrier, inc=1, device_id=peer, device_id_type=MESH)

    loads = []

    def load(src, dst):
        copy = pltpu.make_async_copy(src, dst, load_sem.at[len(loads)])
        copy.start()
        loads.append(copy)

    load(window, win)
    for s in range(SEG):
        load(strain.at[0, s], h.at[s + 1])
    for part in range(3):
        load(ones.at[part % 2], one.at[:, pl.ds(KPAD * part, KPAD)])
    load(twist, twi)
    for part in range(3):
        load(twos.at[:, (0, 0, 1)[part]], two.at[:, pl.ds(256 * part, 256)])
    load(func, fnat)
    load(mask, mnat)

    gap = jnp.zeros((KPAD - HALF, COLS), BF16)
    for parity in range(2):
        for part in range(3):
            rhs[parity, pl.ds(KPAD * part + HALF, KPAD - HALF), :] = gap
    sums[...] = jnp.zeros((16, 128), F32)

    pl.semaphore_wait(barrier, len(neighbours))

    def half_copy(end, p):
        cols = pl.ds(256 * p, 256)
        source, slot, target = ((0, SEG + 1, prev), (SEG - 1, 0, following))[end]
        return pltpu.make_async_remote_copy(
            src_ref=strain.at[0, source, :, cols],
            dst_ref=h.at[slot, :, cols],
            send_sem=half_send.at[end, p],
            recv_sem=half_recv.at[end, p],
            device_id=(target, det),
            device_id_type=MESH,
        )

    @pl.when(jnp.logical_not(first))
    def _():
        for p in range(2):
            half_copy(0, p).start()

    @pl.when(jnp.logical_not(last))
    def _():
        for p in range(2):
            half_copy(1, p).start()

    def edge_copy(end):
        if end == 0:
            return pltpu.make_async_copy(final.at[0], h.at[SEG + 1], o_sem.at[SEG])
        return pltpu.make_async_copy(strain.at[0, 0], h.at[0], o_sem.at[SEG])

    edges = (last, first)
    for end in range(2):

        @pl.when(edges[end])
        def _(end=end):
            edge_copy(end).start()

    for peer in around:
        pl.semaphore_signal(near_sem, inc=1, device_id=peer, device_id_type=MESH)
    two_away = [
        (peer(lax.rem(mine + d, count)), det) for count, mine, peer in axes if count > 4 for d in (2, count - 2)
    ]

    def report_near():
        pl.semaphore_wait(near_sem, len(around))
        for peer in two_away:
            pl.semaphore_signal(far_sem, inc=1, device_id=peer, device_id_type=MESH)

    def report_far():
        if two_away:
            pl.semaphore_wait(far_sem, len(two_away))

    for copy in loads:
        copy.wait()

    low_lane = lax.broadcasted_iota(jnp.int32, (32, 128), 1) < 64

    blocks = []
    for half in range(2):
        f_half = fnat[pl.ds(half, 32, stride=2), :]
        g_half = f_half * mnat[pl.ds(half, 32, stride=2), :].astype(F32)
        blocks.append(jnp.where(low_lane, f_half, pltpu.roll(g_half, 64, 1)))
        blocks.append(jnp.where(low_lane, pltpu.roll(f_half, 64, 1), g_half))
    fg[...] = jnp.concatenate(blocks, axis=0).T

    def split(value):
        high = value.astype(BF16)
        return high, (value - high.astype(F32)).astype(BF16)

    def transform(s, end=None):
        for p in range(2):
            cols = pl.ds(256 * p, 256)
            if end is not None:

                @pl.when(jnp.logical_not(edges[end]))
                def _():
                    half_copy(end, p).wait_recv()

                if p == 0:

                    @pl.when(edges[end])
                    def _():
                        edge_copy(end).wait()

            def windowed(i, carry):
                rows = pl.ds(pl.multiple_of(16 * i, 16), 16)
                upper = h[s + 1, rows, cols]
                lower = h[s + 2, rows, cols]
                w = win[rows, cols]
                for parity, value in ((0, lower + w * (upper - lower)), (1, w * (upper + lower) - lower)):
                    high, low = split(value)
                    rhs[parity, rows, cols] = high
                    rhs[parity, pl.ds(pl.multiple_of(KPAD + 16 * i, 16), 16), cols] = high
                    rhs[parity, pl.ds(pl.multiple_of(2 * KPAD + 16 * i, 16), 16), cols] = low
                return carry

            lax.fori_loop(0, HALF // 16, windowed, 0)
            y[: 2 * EVEN, cols] = jnp.dot(one[: 2 * EVEN], rhs[0, :, cols], preferred_element_type=F32)
            y[2 * EVEN :, cols] = jnp.dot(one[2 * EVEN :], rhs[1, :, cols], preferred_element_type=F32)

        def turned(real_at, imag_at, i):
            rows = pl.ds(pl.multiple_of(16 * i, 16), 16)
            real = y[pl.ds(pl.multiple_of(16 * i + real_at, 16), 16), :]
            imag = y[pl.ds(pl.multiple_of(16 * i + imag_at, 16), 16), :]
            c = twi[0, rows, :]
            n = twi[1, rows, :]
            zr = real * c + imag * n
            zi = imag * c - real * n
            r0, r1, r2, r3 = (zr[:, 128 * p : 128 * p + 128] for p in range(4))
            i0, i1, i2, i3 = (zi[:, 128 * p : 128 * p + 128] for p in range(4))
            ar, br, cr, dr = r0 + r2, r0 - r2, r1 + r3, r1 - r3
            ai, bi, ci, di = i0 + i2, i0 - i2, i1 + i3, i1 - i3
            quarters = ((ar + cr, ai + ci), (br + di, bi - dr), (ar - cr, ai - ci), (br - di, bi + dr))
            for q, pair in enumerate(quarters):
                for at, z in zip((0, 128), pair):
                    high, low = split(z)
                    lhs[q, rows, pl.ds(at, 128)] = high
                    lhs[q, rows, pl.ds(256 + at, 128)] = low
                    lhs[q, rows, pl.ds(512 + at, 128)] = high

        def turned_even(i, carry):
            turned(0, EVEN, i)
            return carry

        def turned_odd(i, carry):
            turned(EVEN, ROWS, i)
            return carry

        lax.fori_loop(0, EVEN // 16, turned_even, 0)
        lax.fori_loop(EVEN // 16, ROWS // 16, turned_odd, 0)
        for pair in range(2):
            for q in (2 * pair, 2 * pair + 1):
                out = jnp.dot(lhs[q], two[q], preferred_element_type=F32)
                xb[s + 1, 0, q] = out[:, :128]
                xb[s + 1, 1, q] = out[:, 128:]
            x_copy(s, pair).start()

    def x_copy(s, pair):
        return pltpu.make_async_remote_copy(
            src_ref=xb.at[s + 1, 1 - det, pl.ds(2 * pair, 2)], dst_ref=rb.at[s + 1, pl.ds(2 * pair, 2)],
            send_sem=x_send.at[s + 1, pair], recv_sem=x_recv.at[s + 1, pair],
            device_id=(me, 1 - det), device_id_type=MESH,
        )

    sign = 1.0 - 2.0 * det.astype(F32)
    group = lax.broadcasted_iota(jnp.int32, (64, 128), 1) // 32
    lane_sign = jnp.where(group < 2, sign, -sign)
    sublane = lax.broadcasted_iota(jnp.int32, (8, 128), 0)
    inner = lax.broadcasted_iota(jnp.int32, (48, 128), 0) < 31

    def reverse_rows(x):
        out = []
        for i in reversed(range(8)):
            v = pltpu.roll(x[8 * i : 8 * i + 8], 4, 0)
            v = jnp.where((sublane & 2) == 0, pltpu.roll(v, 6, 0), pltpu.roll(v, 2, 0))
            out.append(jnp.where((sublane & 1) == 0, pltpu.roll(v, 7, 0), pltpu.roll(v, 1, 0)))
        return jnp.concatenate(out, axis=0)

    def coarse(product, fold):
        direct = mirrored = direct_0 = mirrored_0 = None
        for q in range(4):
            body = product(q, 48, 64) + product(q, 112, 64)
            body = fold(jnp.concatenate([body[:32] + product(q, 176, 32), body[32:]], axis=0))
            zero = fold(product(q, 0, 48))
            if q == 0:
                direct = mirrored = body
                direct_0 = mirrored_0 = zero
            else:
                direct = jnp.where(group == q, body, direct)
                mirrored = jnp.where(group == 3 - q, body, mirrored)
                direct_0 = jnp.where(group[:48] == q, zero, direct_0)
                mirrored_0 = jnp.where(group[:48] == 3 - q, zero, mirrored_0)
        mirrored_0 = jnp.where(inner, pltpu.roll(mirrored_0, 47, 0), 0.0)
        direct = jnp.concatenate([direct[:48] + direct_0, direct[48:]], axis=0)
        mirrored = jnp.concatenate([mirrored[:48] + mirrored_0, mirrored[48:]], axis=0)
        return direct, reverse_rows(mirrored)

    def plus(x):
        return x + pltpu.roll(x, 64, 1)

    def minus(x):
        return x - pltpu.roll(x, 64, 1)

    def crossed(s):
        def mine(q, at, count):
            return xb[s + 1, det, q, pl.ds(at, count), :]

        def theirs(q, at, count):
            return rb[s + 1, q, pl.ds(at, count), :]

        direct, mirrored = coarse(lambda *where: mine(*where) * mine(*where), plus)
        pw[s + 1, 0] = direct + mirrored
        for pair in range(2):
            x_copy(s, pair).wait_recv()
        direct, mirrored = coarse(lambda *where: theirs(*where) * theirs(*where), plus)
        pw[s + 1, 1] = direct + mirrored
        if s < 0:
            return
        direct, mirrored = coarse(lambda *where: mine(*where) * theirs(*where), plus)
        real = direct + mirrored
        re_c[s] = real
        direct, mirrored = coarse(lambda *where: mine(*where) * pltpu.roll(theirs(*where), 64, 1), minus)
        imag = (direct - mirrored) * lane_sign
        turned = jnp.concatenate([real, imag], axis=0).T
        for half in range(2):
            first_part = turned[64 * half : 64 * half + 32]
            second_part = turned[64 * half + 32 : 64 * half + 64]
            ob[s, pl.ds(2 * half, 32, stride=4), :] = jnp.where(low_lane, first_part, pltpu.roll(second_part, 64, 1))
            ob[s, pl.ds(2 * half + 1, 32, stride=4), :] = jnp.where(
                low_lane, pltpu.roll(first_part, 64, 1), second_part
            )
        out_copy(s).start()

    def out_copy(s):
        return pltpu.make_async_copy(ob.at[s], csd.at[s], o_sem.at[s])

    power_copy = pltpu.make_async_remote_copy(
        src_ref=pw.at[1], dst_ref=halo, send_sem=p_sem.at[0], recv_sem=p_sem.at[1],
        device_id=(prev, det), device_id_type=MESH,
    )

    transform(0)
    transform(1)
    report_near()
    crossed(0)
    transform(2)
    report_far()
    crossed(1)
    crossed(2)
    transform(SEG - 1, 0)
    power_copy.start()
    transform(-1, 1)
    crossed(SEG - 1)

    f_t = fg[pl.ds(0, 64), :]
    g_t = fg[pl.ds(64, 64), :]

    def accumulate(s, left, right, weight_left, weight_right):
        mean_a = left(0) * weight_left + right(0) * weight_right
        mean_b = left(1) * weight_left + right(1) * weight_right
        filt = g_t / (mean_a * mean_b)
        sums[pl.ds(s, 1), :] = jnp.sum(filt * re_c[s], axis=0, keepdims=True)
        sums[pl.ds(8 + s, 1), :] = jnp.sum(filt * f_t, axis=0, keepdims=True)

    def own(s):
        return lambda a: pw[s + 1, a]

    for s in (1, 2):
        accumulate(s, own(s - 1), own(s + 1), 0.5, 0.5)
    crossed(-1)
    starts = jnp.where(first, 1.0, 0.5).astype(F32)
    accumulate(0, own(-1), own(1), 1.0 - starts, starts)
    power_copy.wait_recv()
    ends = jnp.where(last, 1.0, 0.5).astype(F32)
    accumulate(SEG - 1, own(SEG - 2), lambda a: halo[a], ends, 1.0 - ends)

    sum_copy = pltpu.make_async_remote_copy(
        src_ref=sums, dst_ref=rsums, send_sem=s_sem.at[0], recv_sem=s_sem.at[1],
        device_id=(me, 1 - det), device_id_type=MESH,
    )
    sum_copy.start()
    lane = lax.broadcasted_iota(jnp.int32, (8, 128), 1)
    row = lax.broadcasted_iota(jnp.int32, (8, 128), 0)
    quality = jnp.zeros((8, 128), F32)
    for s in range(SEG):
        quality = jnp.where(lane == s, flags[s].astype(F32), quality)
    sum_copy.wait_recv()
    whole = jnp.sum(sums[...] + rsums[...], axis=1, keepdims=True)

    def to_lanes(column):
        spread_out = jnp.where(lane == row, jnp.broadcast_to(column, (8, 128)), 0.0)
        return jnp.broadcast_to(jnp.sum(spread_out, axis=0, keepdims=True), (8, 128))

    numerator = to_lanes(whole[:8])
    denominator = to_lanes(whole[8:])
    spread = jnp.sqrt(float(COARSE) / denominator)
    estimate = float(np.sqrt(12.0 * COARSE)) * numerator / denominator
    weight = quality / (spread * spread)
    per_spread = quality / spread
    up = quality * spread
    inside = lane < SEG - 1
    covariance = CORR * up * pltpu.roll(up, 127, 1)
    pair_term = jnp.where(inside, CORR * per_spread * pltpu.roll(per_spread, 127, 1), 0.0)

    rows = [weight, weight * estimate, pair_term, pltpu.roll(per_spread, SEG - 1, 1), per_spread, pltpu.roll(up, SEG - 1, 1)]
    terms = jnp.zeros((8, 128), F32)
    for i, value in enumerate(rows):
        terms = jnp.where(row == i, value, terms)
    terms = jnp.where((lane < SEG) & ((row < 3) | (lane == SEG - 1)), terms, 0.0)
    next_first = jnp.zeros((8, 128), F32)
    open_end = None

    for axis, (count, mine, peer) in enumerate(axes):
        gath[axis, mine] = terms

        def gather_copy(d, axis=axis, count=count, mine=mine, peer=peer):
            return pltpu.make_async_remote_copy(
                src_ref=gath.at[axis, mine], dst_ref=gath.at[axis, mine],
                send_sem=g_send.at[axis, d], recv_sem=g_recv.at[axis, mine],
                device_id=(peer(lax.rem(mine + d, count)), det), device_id_type=MESH,
            )

        for d in range(1, count):
            gather_copy(d).start()
        for d in range(1, count):
            source = lax.rem(mine + d, count)
            pltpu.make_async_remote_copy(
                src_ref=gath.at[axis, source], dst_ref=gath.at[axis, source],
                send_sem=g_send.at[axis, d], recv_sem=g_recv.at[axis, source],
                device_id=(peer(source), det), device_id_type=MESH,
            ).wait_recv()
        groups = [gath[axis, k] for k in range(count)]
        total_terms, joints = groups[0], jnp.zeros((8, 128), F32)
        for before, after in zip(groups[:-1], groups[1:]):
            total_terms = total_terms + after
            joints = joints + before * pltpu.roll(after, 1, 0)
        total_terms = total_terms + jnp.where(row == 2, CORR * pltpu.roll(joints, 6, 0), 0.0)
        terms = jnp.where(row < 3, total_terms, jnp.where(row == 4, groups[-1], groups[0]))
        here = mine < count - 1
        if open_end is not None:
            here = jnp.logical_and(open_end, here)
        next_first = jnp.where(here, gath[axis, jnp.minimum(mine + 1, count - 1)], next_first)
        at_end = mine == count - 1
        open_end = at_end if open_end is None else jnp.logical_and(open_end, at_end)

    covariance = jnp.where(inside, covariance, CORR * up * pltpu.roll(next_first, 5, 0))
    rows3 = jnp.where(row == 0, estimate, jnp.where(row == 1, spread, covariance))
    stats[...] = rows3[:3, :SEG]

    sweep = jnp.sum(terms, axis=1, keepdims=True)
    weight_sum, weighted_sum, pair_sum = sweep[0:1], sweep[1:2], sweep[2:3]
    root = float(np.sqrt(SEG * total))
    pick = lax.broadcasted_iota(jnp.int32, (1, 2), 1)
    combined[...] = jnp.where(
        pick == 0, root * (weighted_sum / weight_sum), root * (jnp.sqrt(weight_sum + 2.0 * pair_sum) / weight_sum)
    )

    for axis, (count, mine, peer) in enumerate(axes):
        for d in range(1, count):
            pltpu.make_async_remote_copy(
                src_ref=gath.at[axis, mine], dst_ref=gath.at[axis, mine],
                send_sem=g_send.at[axis, d], recv_sem=g_recv.at[axis, mine],
                device_id=(peer(lax.rem(mine + d, count)), det), device_id_type=MESH,
            ).wait_send()

    for end in range(2):

        @pl.when(jnp.logical_not(edges[1 - end]))
        def _(end=end):
            for p in range(2):
                half_copy(end, p).wait_send()

    power_copy.wait_send()
    for s in range(SEG):
        out_copy(s).wait()
    for s in range(-1, SEG):
        for pair in range(2):
            x_copy(s, pair).wait_send()
    sum_copy.wait_send()


def writer(csd_in, stats_in, combined_in, csd, stats, combined, csd_v, stats_v, combined_v, sems):
    held = (csd_v, stats_v, combined_v)
    for way, pairs in enumerate((zip((csd_in, stats_in, combined_in), held), zip(held, (csd, stats, combined)))):
        copies = [pltpu.make_async_copy(src, dst, sems.at[way, i]) for i, (src, dst) in enumerate(pairs)]
        for copy in copies:
            copy.start()
        for copy in copies:
            copy.wait()


def on_device(dims, strain, final_half, intersection_function, notch_mask, quality_flags):
    window, ones, twist, twos = tables()
    any_space = pl.BlockSpec(memory_space=pl.ANY)
    hbm = pl.BlockSpec(memory_space=pltpu.HBM)
    vmem = pl.BlockSpec(memory_space=pltpu.VMEM)
    smem = pl.BlockSpec(memory_space=pltpu.SMEM)
    dma = pltpu.SemaphoreType.DMA
    csd, stats, combined = pl.pallas_call(
        functools.partial(kernel, dims),
        out_shape=(
            jax.ShapeDtypeStruct((SEG, 128, 128), F32),
            jax.ShapeDtypeStruct((3, SEG), F32),
            jax.ShapeDtypeStruct((1, 2), F32),
        ),
        in_specs=[hbm, hbm, hbm, hbm, smem, hbm, hbm, hbm, hbm],
        out_specs=(any_space, vmem, vmem),
        scratch_shapes=[
            pltpu.VMEM((SEG + 2, HALF, COLS), F32),
            pltpu.VMEM((HALF, COLS), F32),
            pltpu.VMEM((2 * ROWS, 3 * KPAD), BF16),
            pltpu.VMEM((2, ROWS, COLS), F32),
            pltpu.VMEM((4, 3 * 256, 256), BF16),
            pltpu.VMEM((64, 128), F32),
            pltpu.VMEM((64, 128), jnp.int32),
            pltpu.VMEM((2, 3 * KPAD, COLS), BF16),
            pltpu.VMEM((2 * ROWS, COLS), F32),
            pltpu.VMEM((4, ROWS, 3 * 256), BF16),
            pltpu.VMEM((SEG + 1, 2, 4, ROWS, 128), F32),
            pltpu.VMEM((SEG + 1, 4, ROWS, 128), F32),
            pltpu.VMEM((SEG + 1, 2, 64, 128), F32),
            pltpu.VMEM((2, 64, 128), F32),
            pltpu.VMEM((SEG, 128, 128), F32),
            pltpu.VMEM((16, 128), F32),
            pltpu.VMEM((16, 128), F32),
            pltpu.VMEM((3, 8, 8, 128), F32),
            pltpu.VMEM((128, 128), F32),
            pltpu.VMEM((SEG, 64, 128), F32),
            dma((20,)),
            dma((2, 2)),
            dma((2, 2)),
            dma((SEG + 1, 2)),
            dma((SEG + 1, 2)),
            dma((2,)),
            dma((2,)),
            dma((3, 8)),
            dma((3, 8)),
            dma((SEG + 1,)),
            pltpu.SemaphoreType.REGULAR,
            pltpu.SemaphoreType.REGULAR,
        ],
        compiler_params=pltpu.CompilerParams(
            collective_id=0, has_side_effects=True, vmem_limit_bytes=67_043_328
        ),
    )(
        strain,
        final_half,
        intersection_function.reshape(64, 128),
        notch_mask.reshape(64, 128),
        quality_flags,
        window,
        ones,
        twist,
        twos,
    )
    csd, stats, combined = pl.pallas_call(
        writer,
        out_shape=(
            jax.ShapeDtypeStruct((SEG, 128, 128), F32),
            jax.ShapeDtypeStruct((3, SEG), F32),
            jax.ShapeDtypeStruct((1, 2), F32),
        ),
        in_specs=[any_space] * 3,
        out_specs=[any_space] * 3,
        scratch_shapes=[
            pltpu.VMEM((SEG, 128, 128), F32),
            pltpu.VMEM((3, SEG), F32),
            pltpu.VMEM((1, 2), F32),
            dma((2, 3)),
        ],
    )(csd, stats, combined)
    csd = csd.reshape(SEG, 64, 2, 128).transpose(0, 2, 1, 3).reshape(SEG, 2, 64 * 128)
    return csd, stats, combined.reshape(2)


def solution(mesh):
    count = mesh.shape["tm"]
    dims = (4, 8, 8) if count == 256 else (2, 2, count // 4)
    return jax.shard_map(
        functools.partial(on_device, dims),
        mesh=mesh,
        in_specs=(P("det", "tm", None, None), P("det", None, None), P("det"), P("det"), P("tm")),
        out_specs=(P("tm", None, "det"), P(None, "tm"), P()),
        check_vma=False,
    )
```

```python
import functools

import jax
import jax.numpy as jnp
import numpy as np
from jax import lax
from jax.experimental import pallas as pl
from jax.experimental.pallas import tpu as pltpu
from jax.sharding import PartitionSpec as P

MESH = pl.DeviceIdType.MESH
F32 = jnp.float32
BF16 = jnp.bfloat16

HALF = 192
FULL = 384
COLS = 512
LENGTH = FULL * COLS
KBLK = 256
BIN = 6
GROUPS = FULL // BIN
COARSE = 16384
KPAD = 256
CORR = 27.0 / 154.0
SEG = 4
EVEN, ODD = 112, 96
ROWS = EVEN + ODD


def split_np(table):
    high = table.astype(np.float32).astype(BF16)
    low = (table - high.astype(np.float64)).astype(np.float32).astype(BF16)
    return high, low


@functools.cache
def tables():
    row = np.arange(HALF)
    col = np.arange(COLS)
    window = np.sin(np.pi * (row[:, None] * COLS + col[None, :]) / LENGTH) ** 2

    ones, twists = [], []
    for slabs in (((0, 48, 33), (2, 64, 64)), ((1, 64, 64), (3, 32, 32))):
        bins = np.concatenate([BIN * np.arange(rows) + r for r, rows, _ in slabs])
        keep = np.concatenate([np.arange(rows) < used for _, rows, used in slabs])[:, None]
        angle = 2.0 * np.pi * (bins[:, None] * row[None, :] % FULL) / FULL
        one = np.concatenate([np.cos(angle) * keep, -np.sin(angle) * keep], axis=0)
        ones.append(np.pad(one, ((0, 0), (0, KPAD - HALF))))
        turn = 2.0 * np.pi * (bins[:, None] * col[None, :] % LENGTH) / LENGTH
        twists.append(np.stack([np.cos(turn), np.sin(turn)]))
    one_hi, one_lo = split_np(np.concatenate(ones))

    twos = []
    t = np.arange(32)
    for q in range(4):
        parts = []
        for band in range(2):
            direct, mirrored = 32 * band + t, 127 - 32 * band - t
            k2 = 4 * np.concatenate([direct, mirrored] if q % 2 == 0 else [mirrored, direct]) + q
            angle = 2.0 * np.pi * (np.arange(128)[:, None] * k2[None, :] % COLS) / COLS
            c, s = np.cos(angle), np.sin(angle)
            parts.append(np.concatenate([c, s], axis=0))
            parts.append(np.concatenate([-s, c], axis=0))
        twos.append(np.concatenate(parts, axis=1))
    two_hi, two_lo = split_np(np.stack(twos) * (8.0 / (3.0 * LENGTH) / BIN) ** 0.5)
    return (
        window.astype(np.float32),
        np.stack([one_hi, one_lo]),
        np.concatenate(twists, axis=1).astype(np.float32),
        np.stack([two_hi, two_lo], axis=1),
    )


def kernel(
    dims,
    strain, final, func, mask, flags_in, window, ones, twist, twos,
    csd, stats, combined,
    h, win, one, twi, two, fnat, mnat, rhs, y, lhs, xb, rb, pw, halo, ob, sums, rsums, gath, fg, re_c, flags,
    load_sem, half_send, half_recv, x_send, x_recv, p_sem, s_sem, g_send, g_recv, o_sem, near_sem, far_sem,
):
    nx, nz, ny = dims
    total = nx * nz * ny
    me = lax.axis_index("tm")
    det = lax.axis_index("det")
    cy = lax.rem(me, ny)
    cz = lax.rem(me // ny, nz)
    cx = me // (ny * nz)
    prev = lax.rem(me + total - 1, total)
    following = lax.rem(me + 1, total)
    first = me == 0
    last = me == total - 1

    def y_peer(k):
        return (cx * nz + cz) * ny + k

    def z_peer(k):
        return (cx * nz + k) * ny + cy

    def x_peer(k):
        return (k * nz + cz) * ny + cy

    axes = ((ny, cy, y_peer), (nz, cz, z_peer), (nx, cx, x_peer))

    barrier = pltpu.get_barrier_semaphore()
    around = [(peer(lax.rem(mine + d, count)), det) for count, mine, peer in axes for d in (1, count - 1)]
    neighbours = [(prev, det), (following, det), (me, 1 - det)] + around
    for peer in neighbours:
        pl.semaphore_signal(barrier, inc=1, device_id=peer, device_id_type=MESH)

    loads = []

    def load(src, dst):
        copy = pltpu.make_async_copy(src, dst, load_sem.at[len(loads)])
        copy.start()
        loads.append(copy)
        return copy

    outgoing = [load(strain.at[0, s], h.at[s + 1]) for s in (0, SEG - 1)]
    early = [load(window, win), load(strain.at[0, 1], h.at[2])]
    early += [load(ones.at[part % 2], one.at[:, pl.ds(KPAD * part, KPAD)]) for part in range(3)]
    twist_load = load(twist, twi)
    two_loads = [load(twos.at[:, (0, 0, 1)[part]], two.at[:, pl.ds(256 * part, 256)]) for part in range(3)]
    late = [load(strain.at[0, s], h.at[s + 1]) for s in range(2, SEG - 1)]
    late += [load(func, fnat), load(mask, mnat), load(flags_in, flags)]

    gap = jnp.zeros((KPAD - HALF, COLS), BF16)
    for parity in range(2):
        for part in range(3):
            rhs[parity, pl.ds(KPAD * part + HALF, KPAD - HALF), :] = gap
    sums[...] = jnp.zeros((16, 128), F32)

    pl.semaphore_wait(barrier, len(neighbours))

    def half_copy(end, p):
        cols = pl.ds(256 * p, 256)
        source, slot, target = ((0, SEG + 1, prev), (SEG - 1, 0, following))[end]
        return pltpu.make_async_remote_copy(
            src_ref=h.at[source + 1, :, cols],
            dst_ref=h.at[slot, :, cols],
            send_sem=half_send.at[end, p],
            recv_sem=half_recv.at[end, p],
            device_id=(target, det),
            device_id_type=MESH,
        )

    for copy in outgoing:
        copy.wait()

    @pl.when(jnp.logical_not(first))
    def _():
        for p in range(2):
            half_copy(0, p).start()

    @pl.when(jnp.logical_not(last))
    def _():
        for p in range(2):
            half_copy(1, p).start()

    def edge_copy(end):
        if end == 0:
            return pltpu.make_async_copy(final.at[0], h.at[SEG + 1], o_sem.at[SEG])
        return pltpu.make_async_copy(strain.at[0, 0], h.at[0], o_sem.at[SEG])

    edges = (last, first)
    for end in range(2):

        @pl.when(edges[end])
        def _(end=end):
            edge_copy(end).start()

    for peer in around:
        pl.semaphore_signal(near_sem, inc=1, device_id=peer, device_id_type=MESH)
    two_away = [
        (peer(lax.rem(mine + d, count)), det) for count, mine, peer in axes if count > 4 for d in (2, count - 2)
    ]

    def report_near():
        pl.semaphore_wait(near_sem, len(around))
        for peer in two_away:
            pl.semaphore_signal(far_sem, inc=1, device_id=peer, device_id_type=MESH)

    def report_far():
        if two_away:
            pl.semaphore_wait(far_sem, len(two_away))

    def split(value):
        high = value.astype(BF16)
        return high, (value - high.astype(F32)).astype(BF16)

    def first_stage(s, p, slot=0, end=None):
        cols = pl.ds(256 * p, 256)
        if end is not None:

            @pl.when(jnp.logical_not(edges[end]))
            def _():
                half_copy(end, p).wait_recv()

            if p == 0:

                @pl.when(edges[end])
                def _():
                    edge_copy(end).wait()

        def windowed(i, carry):
            rows = pl.ds(16 * i, 16)
            upper = h[s + 1, rows, cols]
            lower = h[s + 2, rows, cols]
            w = win[rows, cols]
            for parity, value in ((0, lower + w * (upper - lower)), (1, w * (upper + lower) - lower)):
                high, low = split(value)
                rhs[parity, rows, cols] = high
                rhs[parity, pl.ds(KPAD + 16 * i, 16), cols] = high
                rhs[parity, pl.ds(2 * KPAD + 16 * i, 16), cols] = low
            return carry

        for i in range(HALF // 16):
            windowed(i, 0)
        y[slot, : 2 * EVEN, cols] = jnp.dot(one[: 2 * EVEN], rhs[0, :, cols], preferred_element_type=F32)
        y[slot, 2 * EVEN :, cols] = jnp.dot(one[2 * EVEN :], rhs[1, :, cols], preferred_element_type=F32)

    def second_stage(s, slot=0):
        def turned(real_at, imag_at, i):
            rows = pl.ds(16 * i, 16)
            real = y[slot, pl.ds(16 * i + real_at, 16), :]
            imag = y[slot, pl.ds(16 * i + imag_at, 16), :]
            c = twi[0, rows, :]
            n = twi[1, rows, :]
            zr = real * c + imag * n
            zi = imag * c - real * n
            r0, r1, r2, r3 = (zr[:, 128 * p : 128 * p + 128] for p in range(4))
            i0, i1, i2, i3 = (zi[:, 128 * p : 128 * p + 128] for p in range(4))
            ar, br, cr, dr = r0 + r2, r0 - r2, r1 + r3, r1 - r3
            ai, bi, ci, di = i0 + i2, i0 - i2, i1 + i3, i1 - i3
            quarters = ((ar + cr, ai + ci), (br + di, bi - dr), (ar - cr, ai - ci), (br - di, bi + dr))
            for q, pair in enumerate(quarters):
                for at, z in zip((0, 128), pair):
                    high, low = split(z)
                    lhs[q, rows, pl.ds(at, 128)] = high
                    lhs[q, rows, pl.ds(256 + at, 128)] = low
                    lhs[q, rows, pl.ds(512 + at, 128)] = high

        def turned_even(i, carry):
            turned(0, EVEN, i)
            return carry

        def turned_odd(i, carry):
            turned(EVEN, ROWS, i)
            return carry

        for i in range(ROWS // 16):
            (turned_even if i < EVEN // 16 else turned_odd)(i, 0)
        for pair in range(2):
            for q in (2 * pair, 2 * pair + 1):
                out = jnp.dot(lhs[q], two[q], preferred_element_type=F32)
                xb[s + 1, 0, q] = out[:, :128]
                xb[s + 1, 1, q] = out[:, 128:]
            x_copy(s, pair).start()

    def x_copy(s, pair):
        return pltpu.make_async_remote_copy(
            src_ref=xb.at[s + 1, 1 - det, pl.ds(2 * pair, 2)], dst_ref=rb.at[s + 1, pl.ds(2 * pair, 2)],
            send_sem=x_send.at[s + 1, pair], recv_sem=x_recv.at[s + 1, pair],
            device_id=(me, 1 - det), device_id_type=MESH,
        )

    low_lane = lax.broadcasted_iota(jnp.int32, (32, 128), 1) < 64
    sign = 1.0 - 2.0 * det.astype(F32)
    group = lax.broadcasted_iota(jnp.int32, (64, 128), 1) // 32
    lane_sign = jnp.where(group < 2, sign, -sign)
    sublane = lax.broadcasted_iota(jnp.int32, (8, 128), 0)
    inner = lax.broadcasted_iota(jnp.int32, (48, 128), 0) < 31

    def reverse_rows(x):
        out = []
        for i in reversed(range(8)):
            v = pltpu.roll(x[8 * i : 8 * i + 8], 4, 0)
            v = jnp.where((sublane & 2) == 0, pltpu.roll(v, 6, 0), pltpu.roll(v, 2, 0))
            out.append(jnp.where((sublane & 1) == 0, pltpu.roll(v, 7, 0), pltpu.roll(v, 1, 0)))
        return jnp.concatenate(out, axis=0)

    def coarse(product, fold):
        direct = mirrored = direct_0 = mirrored_0 = None
        for q in range(4):
            body = product(q, 48, 64) + product(q, 112, 64)
            body = fold(jnp.concatenate([body[:32] + product(q, 176, 32), body[32:]], axis=0))
            zero = fold(product(q, 0, 48))
            if q == 0:
                direct = mirrored = body
                direct_0 = mirrored_0 = zero
            else:
                direct = jnp.where(group == q, body, direct)
                mirrored = jnp.where(group == 3 - q, body, mirrored)
                direct_0 = jnp.where(group[:48] == q, zero, direct_0)
                mirrored_0 = jnp.where(group[:48] == 3 - q, zero, mirrored_0)
        mirrored_0 = jnp.where(inner, pltpu.roll(mirrored_0, 47, 0), 0.0)
        direct = jnp.concatenate([direct[:48] + direct_0, direct[48:]], axis=0)
        mirrored = jnp.concatenate([mirrored[:48] + mirrored_0, mirrored[48:]], axis=0)
        return direct, reverse_rows(mirrored)

    def plus(x):
        return x + pltpu.roll(x, 64, 1)

    def minus(x):
        return x - pltpu.roll(x, 64, 1)

    def spectra(s):
        def mine(q, at, count):
            return xb[s + 1, det, q, pl.ds(at, count), :]

        def theirs(q, at, count):
            return rb[s + 1, q, pl.ds(at, count), :]

        return mine, theirs

    def crossed(s):
        mine, theirs = spectra(s)
        direct, mirrored = coarse(lambda *where: mine(*where) * mine(*where), plus)
        pw[s + 1, 0] = direct + mirrored
        for pair in range(2):
            x_copy(s, pair).wait_recv()
        direct, mirrored = coarse(lambda *where: theirs(*where) * theirs(*where), plus)
        pw[s + 1, 1] = direct + mirrored
        if s < 0:
            return
        direct, mirrored = coarse(lambda *where: mine(*where) * theirs(*where), plus)
        re_c[s] = direct + mirrored

    def finished(s):
        mine, theirs = spectra(s)
        direct, mirrored = coarse(lambda *where: mine(*where) * pltpu.roll(theirs(*where), 64, 1), minus)
        imag = (direct - mirrored) * lane_sign
        turned = jnp.concatenate([re_c[s], imag], axis=0).T
        for half in range(2):
            first_part = turned[64 * half : 64 * half + 32]
            second_part = turned[64 * half + 32 : 64 * half + 64]
            ob[s, pl.ds(2 * half, 32, stride=4), :] = jnp.where(low_lane, first_part, pltpu.roll(second_part, 64, 1))
            ob[s, pl.ds(2 * half + 1, 32, stride=4), :] = jnp.where(
                low_lane, pltpu.roll(first_part, 64, 1), second_part
            )
        out_copy(s).start()

    def out_copy(s):
        return pltpu.make_async_copy(ob.at[s], csd.at[s], o_sem.at[s])

    power_copy = pltpu.make_async_remote_copy(
        src_ref=pw.at[1], dst_ref=halo, send_sem=p_sem.at[0], recv_sem=p_sem.at[1],
        device_id=(prev, det), device_id_type=MESH,
    )

    for copy in early:
        copy.wait()
    first_stage(0, 0)
    first_stage(0, 1)
    twist_load.wait()
    for copy in two_loads:
        copy.wait()
    second_stage(0)
    for copy in late:
        copy.wait()
    first_stage(1, 0)
    first_stage(1, 1)
    second_stage(1)
    report_near()
    crossed(0)
    power_copy.start()
    first_stage(2, 0)
    first_stage(2, 1)
    second_stage(2)
    report_far()
    first_stage(-1, 0, 2, 1)
    first_stage(SEG - 1, 0, 1, 0)
    crossed(1)
    crossed(2)


    blocks = []
    for half in range(2):
        f_half = fnat[pl.ds(half, 32, stride=2), :]
        g_half = f_half * mnat[pl.ds(half, 32, stride=2), :].astype(F32)
        blocks.append(jnp.where(low_lane, f_half, pltpu.roll(g_half, 64, 1)))
        blocks.append(jnp.where(low_lane, pltpu.roll(f_half, 64, 1), g_half))
    fg[...] = jnp.concatenate(blocks, axis=0).T
    first_stage(-1, 1, 2, 1)
    second_stage(-1, 2)
    first_stage(SEG - 1, 1, 1, 0)
    second_stage(SEG - 1, 1)
    crossed(-1)

    f_t = fg[pl.ds(0, 64), :]
    g_t = fg[pl.ds(64, 64), :]

    def accumulate(s, left, right, weight_left, weight_right):
        mean_a = left(0) * weight_left + right(0) * weight_right
        mean_b = left(1) * weight_left + right(1) * weight_right
        filt = g_t / (mean_a * mean_b)
        sums[pl.ds(s, 1), :] = jnp.sum(filt * re_c[s], axis=0, keepdims=True)
        sums[pl.ds(8 + s, 1), :] = jnp.sum(filt * f_t, axis=0, keepdims=True)

    def own(s):
        return lambda a: pw[s + 1, a]

    starts = jnp.where(first, 1.0, 0.5).astype(F32)
    ends = jnp.where(last, 1.0, 0.5).astype(F32)
    accumulate(1, own(0), own(2), 0.5, 0.5)
    accumulate(0, own(-1), own(1), 1.0 - starts, starts)
    power_copy.wait_recv()
    crossed(SEG - 1)
    accumulate(SEG - 1, own(SEG - 2), lambda a: halo[a], ends, 1.0 - ends)
    accumulate(SEG - 2, own(SEG - 3), own(SEG - 1), 0.5, 0.5)

    sum_copy = pltpu.make_async_remote_copy(
        src_ref=sums, dst_ref=rsums, send_sem=s_sem.at[0], recv_sem=s_sem.at[1],
        device_id=(me, 1 - det), device_id_type=MESH,
    )
    sum_copy.start()
    lane = lax.broadcasted_iota(jnp.int32, (8, 128), 1)
    row = lax.broadcasted_iota(jnp.int32, (8, 128), 0)
    quality = jnp.zeros((8, 128), F32)
    for s in range(SEG):
        quality = jnp.where(lane == s, flags[s].astype(F32), quality)
    sum_copy.wait_recv()
    whole = jnp.sum(sums[...] + rsums[...], axis=1, keepdims=True)

    def to_lanes(column):
        spread_out = jnp.where(lane == row, jnp.broadcast_to(column, (8, 128)), 0.0)
        return jnp.broadcast_to(jnp.sum(spread_out, axis=0, keepdims=True), (8, 128))

    numerator = to_lanes(whole[:8])
    denominator = to_lanes(whole[8:])
    spread = jnp.sqrt(float(COARSE) / denominator)
    estimate = float(np.sqrt(12.0 * COARSE)) * numerator / denominator
    weight = quality / (spread * spread)
    per_spread = quality / spread
    up = quality * spread
    inside = lane < SEG - 1
    covariance = CORR * up * pltpu.roll(up, 127, 1)
    pair_term = jnp.where(inside, CORR * per_spread * pltpu.roll(per_spread, 127, 1), 0.0)

    rows = [weight, weight * estimate, pair_term, pltpu.roll(per_spread, SEG - 1, 1), per_spread, pltpu.roll(up, SEG - 1, 1)]
    terms = jnp.zeros((8, 128), F32)
    for i, value in enumerate(rows):
        terms = jnp.where(row == i, value, terms)
    terms = jnp.where((lane < SEG) & ((row < 3) | (lane == SEG - 1)), terms, 0.0)
    next_first = jnp.zeros((8, 128), F32)
    open_end = None

    for axis, (count, mine, peer) in enumerate(axes):
        gath[axis, mine] = terms

        def gather_copy(d, axis=axis, count=count, mine=mine, peer=peer):
            return pltpu.make_async_remote_copy(
                src_ref=gath.at[axis, mine], dst_ref=gath.at[axis, mine],
                send_sem=g_send.at[axis, d], recv_sem=g_recv.at[axis, mine],
                device_id=(peer(lax.rem(mine + d, count)), det), device_id_type=MESH,
            )

        for d in range(1, count):
            gather_copy(d).start()
        for s in ((0, 1), (2, 3), ())[axis]:
            finished(s)
        for d in range(1, count):
            source = lax.rem(mine + d, count)
            pltpu.make_async_remote_copy(
                src_ref=gath.at[axis, source], dst_ref=gath.at[axis, source],
                send_sem=g_send.at[axis, d], recv_sem=g_recv.at[axis, source],
                device_id=(peer(source), det), device_id_type=MESH,
            ).wait_recv()
        groups = [gath[axis, k] for k in range(count)]
        total_terms, joints = groups[0], jnp.zeros((8, 128), F32)
        for before, after in zip(groups[:-1], groups[1:]):
            total_terms = total_terms + after
            joints = joints + before * pltpu.roll(after, 1, 0)
        total_terms = total_terms + jnp.where(row == 2, CORR * pltpu.roll(joints, 6, 0), 0.0)
        terms = jnp.where(row < 3, total_terms, jnp.where(row == 4, groups[-1], groups[0]))
        here = mine < count - 1
        if open_end is not None:
            here = jnp.logical_and(open_end, here)
        next_first = jnp.where(here, gath[axis, jnp.minimum(mine + 1, count - 1)], next_first)
        at_end = mine == count - 1
        open_end = at_end if open_end is None else jnp.logical_and(open_end, at_end)

    covariance = jnp.where(inside, covariance, CORR * up * pltpu.roll(next_first, 5, 0))
    rows3 = jnp.where(row == 0, estimate, jnp.where(row == 1, spread, covariance))
    stats[...] = rows3[:3, :SEG]

    sweep = jnp.sum(terms, axis=1, keepdims=True)
    weight_sum, weighted_sum, pair_sum = sweep[0:1], sweep[1:2], sweep[2:3]
    root = float(np.sqrt(SEG * total))
    pick = lax.broadcasted_iota(jnp.int32, (1, 2), 1)
    combined[...] = jnp.where(
        pick == 0, root * (weighted_sum / weight_sum), root * (jnp.sqrt(weight_sum + 2.0 * pair_sum) / weight_sum)
    )

    for axis, (count, mine, peer) in enumerate(axes):
        for d in range(1, count):
            pltpu.make_async_remote_copy(
                src_ref=gath.at[axis, mine], dst_ref=gath.at[axis, mine],
                send_sem=g_send.at[axis, d], recv_sem=g_recv.at[axis, mine],
                device_id=(peer(lax.rem(mine + d, count)), det), device_id_type=MESH,
            ).wait_send()

    for end in range(2):

        @pl.when(jnp.logical_not(edges[1 - end]))
        def _(end=end):
            for p in range(2):
                half_copy(end, p).wait_send()

    power_copy.wait_send()
    for s in range(SEG):
        out_copy(s).wait()
    for s in range(-1, SEG):
        for pair in range(2):
            x_copy(s, pair).wait_send()
    sum_copy.wait_send()


def writer(csd_in, stats_in, combined_in, csd, stats, combined, csd_v, stats_v, combined_v, sems):
    held = (csd_v, stats_v, combined_v)
    for way, pairs in enumerate((zip((csd_in, stats_in, combined_in), held), zip(held, (csd, stats, combined)))):
        copies = [pltpu.make_async_copy(src, dst, sems.at[way, i]) for i, (src, dst) in enumerate(pairs)]
        for copy in copies:
            copy.start()
        for copy in copies:
            copy.wait()


def on_device(dims, strain, final_half, intersection_function, notch_mask, quality_flags):
    window, ones, twist, twos = tables()
    any_space = pl.BlockSpec(memory_space=pl.ANY)
    hbm = pl.BlockSpec(memory_space=pltpu.HBM)
    vmem = pl.BlockSpec(memory_space=pltpu.VMEM)
    dma = pltpu.SemaphoreType.DMA
    csd, stats, combined = pl.pallas_call(
        functools.partial(kernel, dims),
        out_shape=(
            jax.ShapeDtypeStruct((SEG, 128, 128), F32),
            jax.ShapeDtypeStruct((3, SEG), F32),
            jax.ShapeDtypeStruct((1, 2), F32),
        ),
        in_specs=[hbm] * 9,
        out_specs=(any_space, vmem, vmem),
        scratch_shapes=[
            pltpu.VMEM((SEG + 2, HALF, COLS), F32),
            pltpu.VMEM((HALF, COLS), F32),
            pltpu.VMEM((2 * ROWS, 3 * KPAD), BF16),
            pltpu.VMEM((2, ROWS, COLS), F32),
            pltpu.VMEM((4, 3 * 256, 256), BF16),
            pltpu.VMEM((64, 128), F32),
            pltpu.VMEM((64, 128), jnp.int32),
            pltpu.VMEM((2, 3 * KPAD, COLS), BF16),
            pltpu.VMEM((3, 2 * ROWS, COLS), F32),
            pltpu.VMEM((4, ROWS, 3 * 256), BF16),
            pltpu.VMEM((SEG + 1, 2, 4, ROWS, 128), F32),
            pltpu.VMEM((SEG + 1, 4, ROWS, 128), F32),
            pltpu.VMEM((SEG + 1, 2, 64, 128), F32),
            pltpu.VMEM((2, 64, 128), F32),
            pltpu.VMEM((SEG, 128, 128), F32),
            pltpu.VMEM((16, 128), F32),
            pltpu.VMEM((16, 128), F32),
            pltpu.VMEM((3, 8, 8, 128), F32),
            pltpu.VMEM((128, 128), F32),
            pltpu.VMEM((SEG, 64, 128), F32),
            pltpu.SMEM((SEG,), jnp.int32),
            dma((20,)),
            dma((2, 2)),
            dma((2, 2)),
            dma((SEG + 1, 2)),
            dma((SEG + 1, 2)),
            dma((2,)),
            dma((2,)),
            dma((3, 8)),
            dma((3, 8)),
            dma((SEG + 1,)),
            pltpu.SemaphoreType.REGULAR,
            pltpu.SemaphoreType.REGULAR,
        ],
        compiler_params=pltpu.CompilerParams(
            collective_id=0, has_side_effects=True, vmem_limit_bytes=67_043_328
        ),
    )(
        strain,
        final_half,
        intersection_function.reshape(64, 128),
        notch_mask.reshape(64, 128),
        quality_flags,
        window,
        ones,
        twist,
        twos,
    )
    csd, stats, combined = pl.pallas_call(
        writer,
        out_shape=(
            jax.ShapeDtypeStruct((SEG, 128, 128), F32),
            jax.ShapeDtypeStruct((3, SEG), F32),
            jax.ShapeDtypeStruct((1, 2), F32),
        ),
        in_specs=[any_space] * 3,
        out_specs=[any_space] * 3,
        scratch_shapes=[
            pltpu.VMEM((SEG, 128, 128), F32),
            pltpu.VMEM((3, SEG), F32),
            pltpu.VMEM((1, 2), F32),
            dma((2, 3)),
        ],
    )(csd, stats, combined)
    csd = csd.reshape(SEG, 64, 2, 128).transpose(0, 2, 1, 3).reshape(SEG, 2, 64 * 128)
    return csd, stats, combined.reshape(2)


def solution(mesh):
    count = mesh.shape["tm"]
    dims = (4, 8, 8) if count == 256 else (2, 2, count // 4)
    return jax.shard_map(
        functools.partial(on_device, dims),
        mesh=mesh,
        in_specs=(P("det", "tm", None, None), P("det", None, None), P("det"), P("det"), P("tm")),
        out_specs=(P("tm", None, "det"), P(None, "tm"), P()),
        check_vma=False,
    )
```

```python
import functools

import jax
import jax.numpy as jnp
import numpy as np
from jax import lax
from jax.experimental import pallas as pl
from jax.experimental.pallas import tpu as pltpu
from jax.sharding import PartitionSpec as P

MESH = pl.DeviceIdType.MESH
F32 = jnp.float32
BF16 = jnp.bfloat16

HALF = 192
FULL = 384
COLS = 512
LENGTH = FULL * COLS
KBLK = 256
BIN = 6
GROUPS = FULL // BIN
COARSE = 16384
KPAD = 256
CORR = 27.0 / 154.0
SEG = 4
EVEN, ODD = 112, 96
ROWS = EVEN + ODD


def split_np(table):
    high = table.astype(np.float32).astype(BF16)
    low = (table - high.astype(np.float64)).astype(np.float32).astype(BF16)
    return high, low


@functools.cache
def tables():
    row = np.arange(HALF)
    col = np.arange(COLS)
    window = np.sin(np.pi * (row[:, None] * COLS + col[None, :]) / LENGTH) ** 2

    ones, twists = [], []
    for slabs in (((0, 48, 33), (2, 64, 64)), ((1, 64, 64), (3, 32, 32))):
        bins = np.concatenate([BIN * np.arange(rows) + r for r, rows, _ in slabs])
        keep = np.concatenate([np.arange(rows) < used for _, rows, used in slabs])[:, None]
        angle = 2.0 * np.pi * (bins[:, None] * row[None, :] % FULL) / FULL
        one = np.concatenate([np.cos(angle) * keep, -np.sin(angle) * keep], axis=0)
        ones.append(np.pad(one, ((0, 0), (0, KPAD - HALF))))
        turn = 2.0 * np.pi * (bins[:, None] * col[None, :] % LENGTH) / LENGTH
        twists.append(np.stack([np.cos(turn), np.sin(turn)]))
    one_hi, one_lo = split_np(np.concatenate(ones))

    twos = []
    t = np.arange(32)
    for q in range(4):
        parts = []
        for band in range(2):
            direct, mirrored = 32 * band + t, 127 - 32 * band - t
            k2 = 4 * np.concatenate([direct, mirrored] if q % 2 == 0 else [mirrored, direct]) + q
            angle = 2.0 * np.pi * (np.arange(128)[:, None] * k2[None, :] % COLS) / COLS
            c, s = np.cos(angle), np.sin(angle)
            parts.append(np.concatenate([c, s], axis=0))
            parts.append(np.concatenate([-s, c], axis=0))
        twos.append(np.concatenate(parts, axis=1))
    two_hi, two_lo = split_np(np.stack(twos) * (8.0 / (3.0 * LENGTH) / BIN) ** 0.5)
    return (
        window.astype(np.float32),
        np.stack([one_hi, one_lo]),
        np.concatenate(twists, axis=1).astype(np.float32),
        np.stack([two_hi, two_lo], axis=1),
    )


def kernel(
    dims,
    strain, final, func, mask, flags_in, window, ones, twist, twos,
    csd, stats, combined,
    h, win, one, twi, two, fnat, mnat, rhs, y, lhs, xb, rb, pw, halo, ob, sums, gath, fg, re_c, flags,
    load_sem, half_send, half_recv, x_send, x_recv, p_sem, g_send, g_recv, o_sem, near_sem, far_sem, pair_sem,
):
    nx, nz, ny = dims
    total = nx * nz * ny
    me = lax.axis_index("tm")
    det = lax.axis_index("det")
    cy = lax.rem(me, ny)
    cz = lax.rem(me // ny, nz)
    cx = me // (ny * nz)
    prev = lax.rem(me + total - 1, total)
    following = lax.rem(me + 1, total)
    first = me == 0
    last = me == total - 1

    def y_peer(k):
        return (cx * nz + cz) * ny + k

    def z_peer(k):
        return (cx * nz + k) * ny + cy

    def x_peer(k):
        return (k * nz + cz) * ny + cy

    axes = ((ny, cy, y_peer), (nz, cz, z_peer), (nx, cx, x_peer))

    barrier = pltpu.get_barrier_semaphore()
    around = [(peer(lax.rem(mine + d, count)), det) for count, mine, peer in axes for d in (1, count - 1)]
    neighbours = [(prev, det), (following, det), (me, 1 - det)] + around
    for peer in neighbours:
        pl.semaphore_signal(barrier, inc=1, device_id=peer, device_id_type=MESH)

    loads = []

    def load(src, dst):
        copy = pltpu.make_async_copy(src, dst, load_sem.at[len(loads)])
        copy.start()
        loads.append(copy)
        return copy

    outgoing = [load(strain.at[0, s], h.at[s + 1]) for s in (0, SEG - 1)]
    early = [load(window, win), load(strain.at[0, 1], h.at[2])]
    early += [load(ones.at[part % 2], one.at[:, pl.ds(KPAD * part, KPAD)]) for part in range(3)]
    twist_load = load(twist, twi)
    two_loads = [load(twos.at[:, (0, 0, 1)[part]], two.at[:, pl.ds(256 * part, 256)]) for part in range(3)]
    late = [load(strain.at[0, s], h.at[s + 1]) for s in range(2, SEG - 1)]
    late += [load(func, fnat), load(mask, mnat), load(flags_in, flags)]

    gap = jnp.zeros((KPAD - HALF, COLS), BF16)
    for parity in range(2):
        for part in range(3):
            rhs[parity, pl.ds(KPAD * part + HALF, KPAD - HALF), :] = gap

    pl.semaphore_wait(barrier, len(neighbours))

    def half_copy(end, p):
        cols = pl.ds(256 * p, 256)
        source, slot, target = ((0, SEG + 1, prev), (SEG - 1, 0, following))[end]
        return pltpu.make_async_remote_copy(
            src_ref=h.at[source + 1, :, cols],
            dst_ref=h.at[slot, :, cols],
            send_sem=half_send.at[end, p],
            recv_sem=half_recv.at[end, p],
            device_id=(target, det),
            device_id_type=MESH,
        )

    for copy in outgoing:
        copy.wait()

    @pl.when(jnp.logical_not(first))
    def _():
        for p in range(2):
            half_copy(0, p).start()

    @pl.when(jnp.logical_not(last))
    def _():
        for p in range(2):
            half_copy(1, p).start()

    def edge_copy(end):
        if end == 0:
            return pltpu.make_async_copy(final.at[0], h.at[SEG + 1], o_sem.at[SEG])
        return pltpu.make_async_copy(strain.at[0, 0], h.at[0], o_sem.at[SEG])

    edges = (last, first)
    for end in range(2):

        @pl.when(edges[end])
        def _(end=end):
            edge_copy(end).start()

    for peer in around:
        pl.semaphore_signal(near_sem, inc=1, device_id=peer, device_id_type=MESH)
    two_away = [
        (peer(lax.rem(mine + d, count)), det) for count, mine, peer in axes if count > 4 for d in (2, count - 2)
    ]

    def report_near():
        pl.semaphore_wait(near_sem, len(around))
        for peer in two_away:
            pl.semaphore_signal(far_sem, inc=1, device_id=peer, device_id_type=MESH)

    def report_far():
        if two_away:
            pl.semaphore_wait(far_sem, len(two_away))
        pl.semaphore_signal(pair_sem, inc=1, device_id=(me, 1 - det), device_id_type=MESH)

    def split(value):
        high = value.astype(BF16)
        return high, (value - high.astype(F32)).astype(BF16)

    def first_stage(s, p, slot=0, end=None):
        cols = pl.ds(256 * p, 256)
        if end is not None:

            @pl.when(jnp.logical_not(edges[end]))
            def _():
                half_copy(end, p).wait_recv()

            if p == 0:

                @pl.when(edges[end])
                def _():
                    edge_copy(end).wait()

        def windowed(i, carry):
            rows = pl.ds(16 * i, 16)
            upper = h[s + 1, rows, cols]
            lower = h[s + 2, rows, cols]
            w = win[rows, cols]
            for parity, value in ((0, lower + w * (upper - lower)), (1, w * (upper + lower) - lower)):
                high, low = split(value)
                rhs[parity, rows, cols] = high
                rhs[parity, pl.ds(KPAD + 16 * i, 16), cols] = high
                rhs[parity, pl.ds(2 * KPAD + 16 * i, 16), cols] = low
            return carry

        for i in range(HALF // 16):
            windowed(i, 0)
        y[slot, : 2 * EVEN, cols] = jnp.dot(one[: 2 * EVEN], rhs[0, :, cols], preferred_element_type=F32)
        y[slot, 2 * EVEN :, cols] = jnp.dot(one[2 * EVEN :], rhs[1, :, cols], preferred_element_type=F32)

    def second_stage(s, slot=0):
        def turned(real_at, imag_at, i):
            rows = pl.ds(16 * i, 16)
            real = y[slot, pl.ds(16 * i + real_at, 16), :]
            imag = y[slot, pl.ds(16 * i + imag_at, 16), :]
            c = twi[0, rows, :]
            n = twi[1, rows, :]
            zr = real * c + imag * n
            zi = imag * c - real * n
            r0, r1, r2, r3 = (zr[:, 128 * p : 128 * p + 128] for p in range(4))
            i0, i1, i2, i3 = (zi[:, 128 * p : 128 * p + 128] for p in range(4))
            ar, br, cr, dr = r0 + r2, r0 - r2, r1 + r3, r1 - r3
            ai, bi, ci, di = i0 + i2, i0 - i2, i1 + i3, i1 - i3
            quarters = ((ar + cr, ai + ci), (br + di, bi - dr), (ar - cr, ai - ci), (br - di, bi + dr))
            for q, pair in enumerate(quarters):
                for at, z in zip((0, 128), pair):
                    high, low = split(z)
                    lhs[q, rows, pl.ds(at, 128)] = high
                    lhs[q, rows, pl.ds(256 + at, 128)] = low
                    lhs[q, rows, pl.ds(512 + at, 128)] = high

        def turned_even(i, carry):
            turned(0, EVEN, i)
            return carry

        def turned_odd(i, carry):
            turned(EVEN, ROWS, i)
            return carry

        for i in range(ROWS // 16):
            (turned_even if i < EVEN // 16 else turned_odd)(i, 0)
        for pair in range(2):
            for q in (2 * pair, 2 * pair + 1):
                out = jnp.dot(lhs[q], two[q], preferred_element_type=F32)
                xb[s + 1, 0, q] = out[:, :128]
                xb[s + 1, 1, q] = out[:, 128:]
            x_copy(s, pair).start()

    def x_copy(s, pair):
        return pltpu.make_async_remote_copy(
            src_ref=xb.at[s + 1, 1 - det, pl.ds(2 * pair, 2)], dst_ref=rb.at[s + 1, pl.ds(2 * pair, 2)],
            send_sem=x_send.at[s + 1, pair], recv_sem=x_recv.at[s + 1, pair],
            device_id=(me, 1 - det), device_id_type=MESH,
        )

    low_lane = lax.broadcasted_iota(jnp.int32, (32, 128), 1) < 64
    sign = 1.0 - 2.0 * det.astype(F32)
    group = lax.broadcasted_iota(jnp.int32, (64, 128), 1) // 32
    lane_sign = jnp.where(group < 2, sign, -sign)
    sublane = lax.broadcasted_iota(jnp.int32, (8, 128), 0)
    inner = lax.broadcasted_iota(jnp.int32, (48, 128), 0) < 31

    def reverse_rows(x):
        out = []
        for i in reversed(range(8)):
            v = pltpu.roll(x[8 * i : 8 * i + 8], 4, 0)
            v = jnp.where((sublane & 2) == 0, pltpu.roll(v, 6, 0), pltpu.roll(v, 2, 0))
            out.append(jnp.where((sublane & 1) == 0, pltpu.roll(v, 7, 0), pltpu.roll(v, 1, 0)))
        return jnp.concatenate(out, axis=0)

    def coarse(product, fold):
        direct = mirrored = direct_0 = mirrored_0 = None
        for q in range(4):
            body = product(q, 48, 64) + product(q, 112, 64)
            body = fold(jnp.concatenate([body[:32] + product(q, 176, 32), body[32:]], axis=0))
            zero = fold(product(q, 0, 48))
            if q == 0:
                direct = mirrored = body
                direct_0 = mirrored_0 = zero
            else:
                direct = jnp.where(group == q, body, direct)
                mirrored = jnp.where(group == 3 - q, body, mirrored)
                direct_0 = jnp.where(group[:48] == q, zero, direct_0)
                mirrored_0 = jnp.where(group[:48] == 3 - q, zero, mirrored_0)
        mirrored_0 = jnp.where(inner, pltpu.roll(mirrored_0, 47, 0), 0.0)
        direct = jnp.concatenate([direct[:48] + direct_0, direct[48:]], axis=0)
        mirrored = jnp.concatenate([mirrored[:48] + mirrored_0, mirrored[48:]], axis=0)
        return direct, reverse_rows(mirrored)

    def plus(x):
        return x + pltpu.roll(x, 64, 1)

    def minus(x):
        return x - pltpu.roll(x, 64, 1)

    def spectra(s):
        def mine(q, at, count):
            return xb[s + 1, det, q, pl.ds(at, count), :]

        def theirs(q, at, count):
            return rb[s + 1, q, pl.ds(at, count), :]

        return mine, theirs

    def crossed(s):
        mine, theirs = spectra(s)
        direct, mirrored = coarse(lambda *where: mine(*where) * mine(*where), plus)
        pw[s + 1, 0] = direct + mirrored
        for pair in range(2):
            x_copy(s, pair).wait_recv()
        direct, mirrored = coarse(lambda *where: theirs(*where) * theirs(*where), plus)
        pw[s + 1, 1] = direct + mirrored
        if s < 0:
            return
        direct, mirrored = coarse(lambda *where: mine(*where) * theirs(*where), plus)
        re_c[s] = direct + mirrored

    def finished(s):
        mine, theirs = spectra(s)
        direct, mirrored = coarse(lambda *where: mine(*where) * pltpu.roll(theirs(*where), 64, 1), minus)
        imag = (direct - mirrored) * lane_sign
        turned = jnp.concatenate([re_c[s], imag], axis=0).T
        for half in range(2):
            first_part = turned[64 * half : 64 * half + 32]
            second_part = turned[64 * half + 32 : 64 * half + 64]
            ob[s, pl.ds(2 * half, 32, stride=4), :] = jnp.where(low_lane, first_part, pltpu.roll(second_part, 64, 1))
            ob[s, pl.ds(2 * half + 1, 32, stride=4), :] = jnp.where(
                low_lane, pltpu.roll(first_part, 64, 1), second_part
            )
        out_copy(s).start()

    def out_copy(s):
        return pltpu.make_async_copy(ob.at[s], csd.at[s], o_sem.at[s])

    power_copy = pltpu.make_async_remote_copy(
        src_ref=pw.at[1], dst_ref=halo, send_sem=p_sem.at[0], recv_sem=p_sem.at[1],
        device_id=(prev, det), device_id_type=MESH,
    )

    for copy in early:
        copy.wait()
    first_stage(0, 0)
    first_stage(0, 1)
    twist_load.wait()
    for copy in two_loads:
        copy.wait()
    second_stage(0)
    for copy in late:
        copy.wait()
    first_stage(1, 0)
    first_stage(1, 1)
    second_stage(1)
    report_near()
    crossed(0)
    power_copy.start()
    first_stage(2, 0)
    first_stage(2, 1)
    second_stage(2)
    report_far()
    first_stage(-1, 0, 2, 1)
    first_stage(SEG - 1, 0, 1, 0)
    crossed(1)
    crossed(2)


    blocks = []
    for half in range(2):
        f_half = fnat[pl.ds(half, 32, stride=2), :]
        g_half = f_half * mnat[pl.ds(half, 32, stride=2), :].astype(F32)
        blocks.append(jnp.where(low_lane, f_half, pltpu.roll(g_half, 64, 1)))
        blocks.append(jnp.where(low_lane, pltpu.roll(f_half, 64, 1), g_half))
    fg[...] = jnp.concatenate(blocks, axis=0).T
    first_stage(-1, 1, 2, 1)
    second_stage(-1, 2)
    first_stage(SEG - 1, 1, 1, 0)
    second_stage(SEG - 1, 1)
    crossed(-1)

    f_t = fg[pl.ds(0, 64), :]
    g_t = fg[pl.ds(64, 64), :]

    def accumulate(s, left, right, weight_left, weight_right):
        mean_a = left(0) * weight_left + right(0) * weight_right
        mean_b = left(1) * weight_left + right(1) * weight_right
        filt = g_t / (mean_a * mean_b)
        sums[pl.ds(s, 1), :] = jnp.sum(filt * re_c[s], axis=0, keepdims=True)
        sums[pl.ds(SEG + s, 1), :] = jnp.sum(filt * f_t, axis=0, keepdims=True)

    def own(s):
        return lambda a: pw[s + 1, a]

    starts = jnp.where(first, 1.0, 0.5).astype(F32)
    ends = jnp.where(last, 1.0, 0.5).astype(F32)
    accumulate(1, own(0), own(2), 0.5, 0.5)
    accumulate(0, own(-1), own(1), 1.0 - starts, starts)
    power_copy.wait_recv()
    crossed(SEG - 1)
    accumulate(SEG - 1, own(SEG - 2), lambda a: halo[a], ends, 1.0 - ends)
    accumulate(SEG - 2, own(SEG - 3), own(SEG - 1), 0.5, 0.5)

    pl.semaphore_wait(pair_sem, 1)
    lane = lax.broadcasted_iota(jnp.int32, (8, 128), 1)
    row = lax.broadcasted_iota(jnp.int32, (8, 128), 0)
    whole = jnp.sum(sums[...], axis=1, keepdims=True)
    message = jnp.sum(jnp.where(lane == row, jnp.broadcast_to(whole, (8, 128)), 0.0), axis=0, keepdims=True)
    for s in range(SEG):
        message = jnp.where(lane[:1] == 2 * SEG + s, 0.5 * flags[s].astype(F32), message)

    def row_copy(axis, mine, slot):
        if axis == 0:
            device = (y_peer(lax.rem(slot, ny)), slot // ny)
        else:
            device = (axes[axis][2](slot), det)
        return pltpu.make_async_remote_copy(
            src_ref=gath.at[axis, mine], dst_ref=gath.at[axis, mine],
            send_sem=g_send.at[axis, slot], recv_sem=g_recv.at[axis, mine],
            device_id=device, device_id_type=MESH,
        )

    def exchange(axis, count, mine, message, work):
        gath[axis, mine] = message
        for d in range(1, count):
            row_copy(axis, mine, lax.rem(mine + d, count)).start()
        for s in work:
            finished(s)
        for d in range(1, count):
            slot = lax.rem(mine + d, count)
            pltpu.make_async_remote_copy(
                src_ref=gath.at[axis, slot], dst_ref=gath.at[axis, slot],
                send_sem=g_send.at[axis, slot], recv_sem=g_recv.at[axis, slot],
                device_id=(me, 1 - det), device_id_type=MESH,
            ).wait_recv()

    def rows_of(axis, start, count):
        table = jnp.zeros((8, 128), F32)
        for k in range(count):
            table = jnp.where(row == k, jnp.broadcast_to(gath[axis, start + k], (8, 128)), table)
        return table

    def summed(x):
        return jnp.sum(x, axis=0, keepdims=True)

    def only(condition, x):
        return jnp.where(condition, x, 0.0)

    slot_y = det * ny + cy
    exchange(0, 2 * ny, slot_y, message, (0, 1))
    table = rows_of(0, 0, ny) + rows_of(0, ny, ny)
    denominator = pltpu.roll(table, 128 - SEG, 1)
    quality = pltpu.roll(table, 128 - 2 * SEG, 1)
    spread = jnp.sqrt(float(COARSE) / denominator)
    estimate = float(np.sqrt(12.0 * COARSE)) * table / denominator
    weight = quality / (spread * spread)
    per_spread = quality / spread
    up = quality * spread

    def following_of(x):
        return jnp.where(lane < SEG - 1, pltpu.roll(x, 127, 1), pltpu.roll(pltpu.roll(x, 7, 0), SEG - 1, 1))

    valid = (lane < SEG) & (row < ny)
    has_next = (lane < SEG - 1) | ((lane == SEG - 1) & (row < ny - 1))
    pair_term = only(valid & has_next, CORR * per_spread * following_of(per_spread))
    covariance = only(has_next, CORR * up * following_of(up))
    own_row = row == cy
    estimate_own = summed(only(own_row, estimate))
    spread_own = summed(only(own_row, spread))
    covariance_own = summed(only(own_row, covariance))
    up_own = summed(only(own_row, up))

    message = summed(
        only(valid, weight)
        + pltpu.roll(only(valid, weight * estimate), 4, 1)
        + pltpu.roll(pair_term, 8, 1)
        + only((row == 0) & (lane == 12), pltpu.roll(per_spread, 12, 1))
        + only((row == 0) & (lane == 13), pltpu.roll(up, 13, 1))
        + only((row == ny - 1) & (lane == 14), pltpu.roll(per_spread, 15 - SEG, 1))
    )
    at_end = cy == ny - 1
    next_first = jnp.zeros((1, 128), F32)
    for axis, work in ((1, (2, 3)), (2, ())):
        count, mine, _ = axes[axis]
        exchange(axis, count, mine, message, work)
        table = rows_of(axis, 0, count)
        found = (row == mine + 1) & (row < count) & (lane == 13) & at_end
        next_first = next_first + summed(only(found, table))
        at_end = jnp.logical_and(at_end, mine == count - 1)
        joint = CORR * table * pltpu.roll(pltpu.roll(table, 7, 0), 2, 1)
        message = summed(
            only((lane < 12) | ((row == 0) & (lane < 14)) | ((row == count - 1) & (lane == 14)), table)
            + only((lane == 8) & (row < count - 1), pltpu.roll(joint, 122, 1))
        )

    last_lane = lane[:1] == SEG - 1
    covariance_own = covariance_own + only(last_lane, CORR * up_own * pltpu.roll(next_first, 115 + SEG - 1, 1))
    three = jnp.where(row == 0, estimate_own, jnp.where(row == 1, spread_own, covariance_own))
    stats[...] = three[:3, :SEG]

    def lanes_from(at):
        return jnp.sum(only((lane[:1] >= at) & (lane[:1] < at + 4), message), axis=1, keepdims=True)

    weight_sum, weighted_sum, pair_sum = lanes_from(0), lanes_from(4), lanes_from(8)
    root = float(np.sqrt(SEG * total))
    pick = lax.broadcasted_iota(jnp.int32, (1, 2), 1)
    combined[...] = jnp.where(
        pick == 0, root * (weighted_sum / weight_sum), root * (jnp.sqrt(weight_sum + 2.0 * pair_sum) / weight_sum)
    )

    for axis, count, mine in ((0, 2 * ny, slot_y), (1, nz, cz), (2, nx, cx)):
        for d in range(1, count):
            row_copy(axis, mine, lax.rem(mine + d, count)).wait_send()

    for end in range(2):

        @pl.when(jnp.logical_not(edges[1 - end]))
        def _(end=end):
            for p in range(2):
                half_copy(end, p).wait_send()

    power_copy.wait_send()
    for s in range(SEG):
        out_copy(s).wait()
    for s in range(-1, SEG):
        for pair in range(2):
            x_copy(s, pair).wait_send()


def writer(csd_in, stats_in, combined_in, csd, stats, combined, csd_v, stats_v, combined_v, sems):
    held = (csd_v, stats_v, combined_v)
    for way, pairs in enumerate((zip((csd_in, stats_in, combined_in), held), zip(held, (csd, stats, combined)))):
        copies = [pltpu.make_async_copy(src, dst, sems.at[way, i]) for i, (src, dst) in enumerate(pairs)]
        for copy in copies:
            copy.start()
        for copy in copies:
            copy.wait()


def on_device(dims, strain, final_half, intersection_function, notch_mask, quality_flags):
    window, ones, twist, twos = tables()
    any_space = pl.BlockSpec(memory_space=pl.ANY)
    hbm = pl.BlockSpec(memory_space=pltpu.HBM)
    vmem = pl.BlockSpec(memory_space=pltpu.VMEM)
    dma = pltpu.SemaphoreType.DMA
    csd, stats, combined = pl.pallas_call(
        functools.partial(kernel, dims),
        out_shape=(
            jax.ShapeDtypeStruct((SEG, 128, 128), F32),
            jax.ShapeDtypeStruct((3, SEG), F32),
            jax.ShapeDtypeStruct((1, 2), F32),
        ),
        in_specs=[hbm] * 9,
        out_specs=(any_space, vmem, vmem),
        scratch_shapes=[
            pltpu.VMEM((SEG + 2, HALF, COLS), F32),
            pltpu.VMEM((HALF, COLS), F32),
            pltpu.VMEM((2 * ROWS, 3 * KPAD), BF16),
            pltpu.VMEM((2, ROWS, COLS), F32),
            pltpu.VMEM((4, 3 * 256, 256), BF16),
            pltpu.VMEM((64, 128), F32),
            pltpu.VMEM((64, 128), jnp.int32),
            pltpu.VMEM((2, 3 * KPAD, COLS), BF16),
            pltpu.VMEM((3, 2 * ROWS, COLS), F32),
            pltpu.VMEM((4, ROWS, 3 * 256), BF16),
            pltpu.VMEM((SEG + 1, 2, 4, ROWS, 128), F32),
            pltpu.VMEM((SEG + 1, 4, ROWS, 128), F32),
            pltpu.VMEM((SEG + 1, 2, 64, 128), F32),
            pltpu.VMEM((2, 64, 128), F32),
            pltpu.VMEM((SEG, 128, 128), F32),
            pltpu.VMEM((8, 128), F32),
            pltpu.VMEM((3, 16, 1, 128), F32),
            pltpu.VMEM((128, 128), F32),
            pltpu.VMEM((SEG, 64, 128), F32),
            pltpu.SMEM((SEG,), jnp.int32),
            dma((20,)),
            dma((2, 2)),
            dma((2, 2)),
            dma((SEG + 1, 2)),
            dma((SEG + 1, 2)),
            dma((2,)),
            dma((3, 16)),
            dma((3, 16)),
            dma((SEG + 1,)),
            pltpu.SemaphoreType.REGULAR,
            pltpu.SemaphoreType.REGULAR,
            pltpu.SemaphoreType.REGULAR,
        ],
        compiler_params=pltpu.CompilerParams(
            collective_id=0, has_side_effects=True, vmem_limit_bytes=67_043_328
        ),
    )(
        strain,
        final_half,
        intersection_function.reshape(64, 128),
        notch_mask.reshape(64, 128),
        quality_flags,
        window,
        ones,
        twist,
        twos,
    )
    csd, stats, combined = pl.pallas_call(
        writer,
        out_shape=(
            jax.ShapeDtypeStruct((SEG, 128, 128), F32),
            jax.ShapeDtypeStruct((3, SEG), F32),
            jax.ShapeDtypeStruct((1, 2), F32),
        ),
        in_specs=[any_space] * 3,
        out_specs=[any_space] * 3,
        scratch_shapes=[
            pltpu.VMEM((SEG, 128, 128), F32),
            pltpu.VMEM((3, SEG), F32),
            pltpu.VMEM((1, 2), F32),
            dma((2, 3)),
        ],
    )(csd, stats, combined)
    csd = csd.reshape(SEG, 64, 2, 128).transpose(0, 2, 1, 3).reshape(SEG, 2, 64 * 128)
    return csd, stats, combined.reshape(2)


def solution(mesh):
    count = mesh.shape["tm"]
    dims = (4, 8, 8) if count == 256 else (2, 2, count // 4)
    return jax.shard_map(
        functools.partial(on_device, dims),
        mesh=mesh,
        in_specs=(P("det", "tm", None, None), P("det", None, None), P("det"), P("det"), P("tm")),
        out_specs=(P("tm", None, "det"), P(None, "tm"), P()),
        check_vma=False,
    )
```

```python
import functools

import jax
import jax.numpy as jnp
import numpy as np
from jax import lax
from jax.experimental import pallas as pl
from jax.experimental.pallas import tpu as pltpu
from jax.sharding import PartitionSpec as P

MESH = pl.DeviceIdType.MESH
F32 = jnp.float32
BF16 = jnp.bfloat16

HALF = 192
FULL = 384
COLS = 512
LENGTH = FULL * COLS
KBLK = 256
BIN = 6
GROUPS = FULL // BIN
COARSE = 16384
KPAD = 256
CORR = 27.0 / 154.0
SEG = 4
EVEN, ODD = 112, 96
ROWS = EVEN + ODD


def split_np(table):
    high = table.astype(np.float32).astype(BF16)
    low = (table - high.astype(np.float64)).astype(np.float32).astype(BF16)
    return high, low


@functools.cache
def tables():
    row = np.arange(HALF)
    col = np.arange(COLS)
    window = np.sin(np.pi * (row[:, None] * COLS + col[None, :]) / LENGTH) ** 2

    ones, twists = [], []
    for slabs in (((0, 48, 33), (2, 64, 64)), ((1, 64, 64), (3, 32, 32))):
        bins = np.concatenate([BIN * np.arange(rows) + r for r, rows, _ in slabs])
        keep = np.concatenate([np.arange(rows) < used for _, rows, used in slabs])[:, None]
        angle = 2.0 * np.pi * (bins[:, None] * row[None, :] % FULL) / FULL
        one = np.concatenate([np.cos(angle) * keep, -np.sin(angle) * keep], axis=0)
        ones.append(np.pad(one, ((0, 0), (0, KPAD - HALF))))
        turn = 2.0 * np.pi * (bins[:, None] * col[None, :] % LENGTH) / LENGTH
        twists.append(np.stack([np.cos(turn), np.sin(turn)]))
    stacked = [part for one in ones for part in split_np(one)]

    twos = []
    t = np.arange(32)
    for q in range(4):
        parts = []
        for band in range(2):
            direct, mirrored = 32 * band + t, 127 - 32 * band - t
            k2 = 4 * np.concatenate([direct, mirrored] if q % 2 == 0 else [mirrored, direct]) + q
            angle = 2.0 * np.pi * (np.arange(128)[:, None] * k2[None, :] % COLS) / COLS
            c, s = np.cos(angle), np.sin(angle)
            parts.append(np.concatenate([c, s], axis=0))
            parts.append(np.concatenate([-s, c], axis=0))
        twos.append(np.concatenate(parts, axis=1))
    two_hi, two_lo = split_np(np.stack(twos) * (8.0 / (3.0 * LENGTH) / BIN) ** 0.5)
    return (
        window.astype(np.float32),
        np.concatenate(stacked),
        np.concatenate(twists, axis=1).astype(np.float32),
        np.stack([two_hi, two_lo], axis=1),
    )


def kernel(
    dims,
    strain, final, func, mask, flags_in, window, ones, twist, twos,
    csd, stats, combined,
    h, win, one, twi, two, fnat, mnat, rhs, y, lhs, xb, rb, pw, halo, ob, sums, gath, fg, re_c, flags,
    load_sem, half_send, half_recv, x_send, x_recv, p_sem, g_send, g_recv, o_sem, near_sem, far_sem, pair_sem,
):
    nx, nz, ny = dims
    total = nx * nz * ny
    me = lax.axis_index("tm")
    det = lax.axis_index("det")
    cy = lax.rem(me, ny)
    cz = lax.rem(me // ny, nz)
    cx = me // (ny * nz)
    prev = lax.rem(me + total - 1, total)
    following = lax.rem(me + 1, total)
    first = me == 0
    last = me == total - 1

    def y_peer(k):
        return (cx * nz + cz) * ny + k

    def z_peer(k):
        return (cx * nz + k) * ny + cy

    def x_peer(k):
        return (k * nz + cz) * ny + cy

    axes = ((ny, cy, y_peer), (nz, cz, z_peer), (nx, cx, x_peer))

    barrier = pltpu.get_barrier_semaphore()
    around = [(peer(lax.rem(mine + d, count)), det) for count, mine, peer in axes for d in (1, count - 1)]
    neighbours = [(prev, det), (following, det), (me, 1 - det)] + around
    for peer in neighbours:
        pl.semaphore_signal(barrier, inc=1, device_id=peer, device_id_type=MESH)

    loads = []

    def load(src, dst):
        copy = pltpu.make_async_copy(src, dst, load_sem.at[len(loads)])
        copy.start()
        loads.append(copy)
        return copy

    outgoing = [load(strain.at[0, s], h.at[s + 1]) for s in (0, SEG - 1)]
    early = [load(window, win), load(strain.at[0, 1], h.at[2])]
    early.append(load(ones, one))
    twist_load = load(twist, twi)
    two_loads = [load(twos, two)]
    late = [load(strain.at[0, s], h.at[s + 1]) for s in range(2, SEG - 1)]
    late += [load(func, fnat), load(mask, mnat), load(flags_in, flags)]

    gap = jnp.zeros((KPAD - HALF, COLS), BF16)
    for parity in range(2):
        for part in range(2):
            rhs[parity, part, HALF:, :] = gap

    pl.semaphore_wait(barrier, len(neighbours))

    def half_copy(end, p):
        cols = pl.ds(256 * p, 256)
        source, slot, target = ((0, SEG + 1, prev), (SEG - 1, 0, following))[end]
        return pltpu.make_async_remote_copy(
            src_ref=h.at[source + 1, :, cols],
            dst_ref=h.at[slot, :, cols],
            send_sem=half_send.at[end, p],
            recv_sem=half_recv.at[end, p],
            device_id=(target, det),
            device_id_type=MESH,
        )

    for copy in outgoing:
        copy.wait()

    @pl.when(jnp.logical_not(first))
    def _():
        for p in range(2):
            half_copy(0, p).start()

    @pl.when(jnp.logical_not(last))
    def _():
        for p in range(2):
            half_copy(1, p).start()

    def edge_copy(end):
        if end == 0:
            return pltpu.make_async_copy(final.at[0], h.at[SEG + 1], o_sem.at[SEG])
        return pltpu.make_async_copy(strain.at[0, 0], h.at[0], o_sem.at[SEG])

    edges = (last, first)
    for end in range(2):

        @pl.when(edges[end])
        def _(end=end):
            edge_copy(end).start()

    for peer in around:
        pl.semaphore_signal(near_sem, inc=1, device_id=peer, device_id_type=MESH)
    two_away = [
        (peer(lax.rem(mine + d, count)), det) for count, mine, peer in axes if count > 4 for d in (2, count - 2)
    ]

    def report_near():
        pl.semaphore_wait(near_sem, len(around))
        for peer in two_away:
            pl.semaphore_signal(far_sem, inc=1, device_id=peer, device_id_type=MESH)

    def report_far():
        if two_away:
            pl.semaphore_wait(far_sem, len(two_away))
        pl.semaphore_signal(pair_sem, inc=1, device_id=(me, 1 - det), device_id_type=MESH)

    def split(value):
        high = value.astype(BF16)
        return high, (value - high.astype(F32)).astype(BF16)

    def passes(left, right_high, right_low, count):
        both = jnp.dot(left, right_high, preferred_element_type=F32)
        rest = jnp.dot(left[:count], right_low, preferred_element_type=F32)
        return both[:count] + (both[count:] + rest)

    def first_stage(s, p, slot=0, end=None):
        cols = pl.ds(256 * p, 256)
        if end is not None:

            @pl.when(jnp.logical_not(edges[end]))
            def _():
                half_copy(end, p).wait_recv()

            if p == 0:

                @pl.when(edges[end])
                def _():
                    edge_copy(end).wait()

        def windowed(i, carry):
            rows = pl.ds(16 * i, 16)
            upper = h[s + 1, rows, cols]
            lower = h[s + 2, rows, cols]
            w = win[rows, cols]
            for parity, value in ((0, lower + w * (upper - lower)), (1, w * (upper + lower) - lower)):
                high, low = split(value)
                rhs[parity, 0, rows, cols] = high
                rhs[parity, 1, rows, cols] = low
            return carry

        for i in range(HALF // 16):
            windowed(i, 0)
        for parity, at, count in ((0, 0, 2 * EVEN), (1, 2 * EVEN, 2 * ODD)):
            left = one[2 * at : 2 * at + 2 * count]
            y[slot, at : at + count, cols] = passes(left, rhs[parity, 0, :, cols], rhs[parity, 1, :, cols], count)

    def second_stage(s, slot=0):
        def turned(real_at, imag_at, i):
            rows = pl.ds(16 * i, 16)
            real = y[slot, pl.ds(16 * i + real_at, 16), :]
            imag = y[slot, pl.ds(16 * i + imag_at, 16), :]
            c = twi[0, rows, :]
            n = twi[1, rows, :]
            zr = real * c + imag * n
            zi = imag * c - real * n
            r0, r1, r2, r3 = (zr[:, 128 * p : 128 * p + 128] for p in range(4))
            i0, i1, i2, i3 = (zi[:, 128 * p : 128 * p + 128] for p in range(4))
            ar, br, cr, dr = r0 + r2, r0 - r2, r1 + r3, r1 - r3
            ai, bi, ci, di = i0 + i2, i0 - i2, i1 + i3, i1 - i3
            quarters = ((ar + cr, ai + ci), (br + di, bi - dr), (ar - cr, ai - ci), (br - di, bi + dr))
            for q, pair in enumerate(quarters):
                for at, z in zip((0, 128), pair):
                    high, low = split(z)
                    lhs[q, rows, pl.ds(at, 128)] = high
                    lhs[q, pl.ds(ROWS + 16 * i, 16), pl.ds(at, 128)] = low

        def turned_even(i, carry):
            turned(0, EVEN, i)
            return carry

        def turned_odd(i, carry):
            turned(EVEN, ROWS, i)
            return carry

        for i in range(ROWS // 16):
            (turned_even if i < EVEN // 16 else turned_odd)(i, 0)
        for q in range(4):
            out = passes(lhs[q], two[q, 0], two[q, 1], ROWS)
            xb[s + 1, 0, q] = out[:, :128]
            xb[s + 1, 1, q] = out[:, 128:]
        for pair in range(2):
            x_copy(s, pair).start()

    def x_copy(s, pair):
        return pltpu.make_async_remote_copy(
            src_ref=xb.at[s + 1, 1 - det, pl.ds(2 * pair, 2)], dst_ref=rb.at[s + 1, pl.ds(2 * pair, 2)],
            send_sem=x_send.at[s + 1, pair], recv_sem=x_recv.at[s + 1, pair],
            device_id=(me, 1 - det), device_id_type=MESH,
        )

    low_lane = lax.broadcasted_iota(jnp.int32, (32, 128), 1) < 64
    sign = 1.0 - 2.0 * det.astype(F32)
    group = lax.broadcasted_iota(jnp.int32, (64, 128), 1) // 32
    lane_sign = jnp.where(group < 2, sign, -sign)
    sublane = lax.broadcasted_iota(jnp.int32, (8, 128), 0)
    inner = lax.broadcasted_iota(jnp.int32, (48, 128), 0) < 31

    def reverse_rows(x):
        out = []
        for i in reversed(range(8)):
            v = pltpu.roll(x[8 * i : 8 * i + 8], 4, 0)
            v = jnp.where((sublane & 2) == 0, pltpu.roll(v, 6, 0), pltpu.roll(v, 2, 0))
            out.append(jnp.where((sublane & 1) == 0, pltpu.roll(v, 7, 0), pltpu.roll(v, 1, 0)))
        return jnp.concatenate(out, axis=0)

    def coarse(product, fold):
        direct = mirrored = direct_0 = mirrored_0 = None
        for q in range(4):
            body = product(q, 48, 64) + product(q, 112, 64)
            body = fold(jnp.concatenate([body[:32] + product(q, 176, 32), body[32:]], axis=0))
            zero = fold(product(q, 0, 48))
            if q == 0:
                direct = mirrored = body
                direct_0 = mirrored_0 = zero
            else:
                direct = jnp.where(group == q, body, direct)
                mirrored = jnp.where(group == 3 - q, body, mirrored)
                direct_0 = jnp.where(group[:48] == q, zero, direct_0)
                mirrored_0 = jnp.where(group[:48] == 3 - q, zero, mirrored_0)
        mirrored_0 = jnp.where(inner, pltpu.roll(mirrored_0, 47, 0), 0.0)
        direct = jnp.concatenate([direct[:48] + direct_0, direct[48:]], axis=0)
        mirrored = jnp.concatenate([mirrored[:48] + mirrored_0, mirrored[48:]], axis=0)
        return direct, reverse_rows(mirrored)

    def plus(x):
        return x + pltpu.roll(x, 64, 1)

    def minus(x):
        return x - pltpu.roll(x, 64, 1)

    def spectra(s):
        def mine(q, at, count):
            return xb[s + 1, det, q, pl.ds(at, count), :]

        def theirs(q, at, count):
            return rb[s + 1, q, pl.ds(at, count), :]

        return mine, theirs

    def crossed(s):
        mine, theirs = spectra(s)
        direct, mirrored = coarse(lambda *where: mine(*where) * mine(*where), plus)
        pw[s + 1, 0] = direct + mirrored
        for pair in range(2):
            x_copy(s, pair).wait_recv()
        direct, mirrored = coarse(lambda *where: theirs(*where) * theirs(*where), plus)
        pw[s + 1, 1] = direct + mirrored
        if s < 0:
            return
        direct, mirrored = coarse(lambda *where: mine(*where) * theirs(*where), plus)
        re_c[s] = direct + mirrored

    def finished(s):
        mine, theirs = spectra(s)
        direct, mirrored = coarse(lambda *where: mine(*where) * pltpu.roll(theirs(*where), 64, 1), minus)
        imag = (direct - mirrored) * lane_sign
        turned = jnp.concatenate([re_c[s], imag], axis=0).T
        for half in range(2):
            first_part = turned[64 * half : 64 * half + 32]
            second_part = turned[64 * half + 32 : 64 * half + 64]
            ob[s, pl.ds(2 * half, 32, stride=4), :] = jnp.where(low_lane, first_part, pltpu.roll(second_part, 64, 1))
            ob[s, pl.ds(2 * half + 1, 32, stride=4), :] = jnp.where(
                low_lane, pltpu.roll(first_part, 64, 1), second_part
            )
        out_copy(s).start()

    def out_copy(s):
        return pltpu.make_async_copy(ob.at[s], csd.at[s], o_sem.at[s])

    power_copy = pltpu.make_async_remote_copy(
        src_ref=pw.at[1], dst_ref=halo, send_sem=p_sem.at[0], recv_sem=p_sem.at[1],
        device_id=(prev, det), device_id_type=MESH,
    )

    for copy in early:
        copy.wait()
    first_stage(0, 0)
    first_stage(0, 1)
    twist_load.wait()
    for copy in two_loads:
        copy.wait()
    second_stage(0)
    for copy in late:
        copy.wait()
    first_stage(1, 0)
    first_stage(1, 1)
    second_stage(1)
    report_near()
    crossed(0)
    power_copy.start()
    first_stage(2, 0)
    first_stage(2, 1)
    second_stage(2)
    report_far()
    first_stage(-1, 0, 2, 1)
    first_stage(SEG - 1, 0, 1, 0)
    crossed(1)
    crossed(2)


    blocks = []
    for half in range(2):
        f_half = fnat[pl.ds(half, 32, stride=2), :]
        g_half = f_half * mnat[pl.ds(half, 32, stride=2), :].astype(F32)
        blocks.append(jnp.where(low_lane, f_half, pltpu.roll(g_half, 64, 1)))
        blocks.append(jnp.where(low_lane, pltpu.roll(f_half, 64, 1), g_half))
    fg[...] = jnp.concatenate(blocks, axis=0).T
    first_stage(-1, 1, 2, 1)
    second_stage(-1, 2)
    first_stage(SEG - 1, 1, 1, 0)
    second_stage(SEG - 1, 1)
    crossed(-1)

    f_t = fg[pl.ds(0, 64), :]
    g_t = fg[pl.ds(64, 64), :]

    def accumulate(s, left, right, weight_left, weight_right):
        mean_a = left(0) * weight_left + right(0) * weight_right
        mean_b = left(1) * weight_left + right(1) * weight_right
        filt = g_t / (mean_a * mean_b)
        sums[pl.ds(s, 1), :] = jnp.sum(filt * re_c[s], axis=0, keepdims=True)
        sums[pl.ds(SEG + s, 1), :] = jnp.sum(filt * f_t, axis=0, keepdims=True)

    def own(s):
        return lambda a: pw[s + 1, a]

    starts = jnp.where(first, 1.0, 0.5).astype(F32)
    ends = jnp.where(last, 1.0, 0.5).astype(F32)
    accumulate(1, own(0), own(2), 0.5, 0.5)
    accumulate(0, own(-1), own(1), 1.0 - starts, starts)
    power_copy.wait_recv()
    crossed(SEG - 1)
    accumulate(SEG - 1, own(SEG - 2), lambda a: halo[a], ends, 1.0 - ends)
    accumulate(SEG - 2, own(SEG - 3), own(SEG - 1), 0.5, 0.5)

    pl.semaphore_wait(pair_sem, 1)
    lane = lax.broadcasted_iota(jnp.int32, (8, 128), 1)
    row = lax.broadcasted_iota(jnp.int32, (8, 128), 0)
    whole = jnp.sum(sums[...], axis=1, keepdims=True)
    message = jnp.sum(jnp.where(lane == row, jnp.broadcast_to(whole, (8, 128)), 0.0), axis=0, keepdims=True)
    for s in range(SEG):
        message = jnp.where(lane[:1] == 2 * SEG + s, 0.5 * flags[s].astype(F32), message)

    def row_copy(axis, mine, slot):
        if axis == 0:
            device = (y_peer(lax.rem(slot, ny)), slot // ny)
        else:
            device = (axes[axis][2](slot), det)
        return pltpu.make_async_remote_copy(
            src_ref=gath.at[axis, mine], dst_ref=gath.at[axis, mine],
            send_sem=g_send.at[axis, slot], recv_sem=g_recv.at[axis, mine],
            device_id=device, device_id_type=MESH,
        )

    def exchange(axis, count, mine, message, work):
        gath[axis, mine] = message
        for d in range(1, count):
            row_copy(axis, mine, lax.rem(mine + d, count)).start()
        for s in work:
            finished(s)
        for d in range(1, count):
            slot = lax.rem(mine + d, count)
            pltpu.make_async_remote_copy(
                src_ref=gath.at[axis, slot], dst_ref=gath.at[axis, slot],
                send_sem=g_send.at[axis, slot], recv_sem=g_recv.at[axis, slot],
                device_id=(me, 1 - det), device_id_type=MESH,
            ).wait_recv()

    def rows_of(axis, start, count):
        table = jnp.zeros((8, 128), F32)
        for k in range(count):
            table = jnp.where(row == k, jnp.broadcast_to(gath[axis, start + k], (8, 128)), table)
        return table

    def summed(x):
        return jnp.sum(x, axis=0, keepdims=True)

    def only(condition, x):
        return jnp.where(condition, x, 0.0)

    slot_y = det * ny + cy
    exchange(0, 2 * ny, slot_y, message, (0, 1))
    table = rows_of(0, 0, ny) + rows_of(0, ny, ny)
    denominator = pltpu.roll(table, 128 - SEG, 1)
    quality = pltpu.roll(table, 128 - 2 * SEG, 1)
    spread = jnp.sqrt(float(COARSE) / denominator)
    estimate = float(np.sqrt(12.0 * COARSE)) * table / denominator
    weight = quality / (spread * spread)
    per_spread = quality / spread
    up = quality * spread

    def following_of(x):
        return jnp.where(lane < SEG - 1, pltpu.roll(x, 127, 1), pltpu.roll(pltpu.roll(x, 7, 0), SEG - 1, 1))

    valid = (lane < SEG) & (row < ny)
    has_next = (lane < SEG - 1) | ((lane == SEG - 1) & (row < ny - 1))
    pair_term = only(valid & has_next, CORR * per_spread * following_of(per_spread))
    covariance = only(has_next, CORR * up * following_of(up))
    own_row = row == cy
    estimate_own = summed(only(own_row, estimate))
    spread_own = summed(only(own_row, spread))
    covariance_own = summed(only(own_row, covariance))
    up_own = summed(only(own_row, up))

    message = summed(
        only(valid, weight)
        + pltpu.roll(only(valid, weight * estimate), 4, 1)
        + pltpu.roll(pair_term, 8, 1)
        + only((row == 0) & (lane == 12), pltpu.roll(per_spread, 12, 1))
        + only((row == 0) & (lane == 13), pltpu.roll(up, 13, 1))
        + only((row == ny - 1) & (lane == 14), pltpu.roll(per_spread, 15 - SEG, 1))
    )
    at_end = cy == ny - 1
    next_first = jnp.zeros((1, 128), F32)
    for axis, work in ((1, (2, 3)), (2, ())):
        count, mine, _ = axes[axis]
        exchange(axis, count, mine, message, work)
        table = rows_of(axis, 0, count)
        found = (row == mine + 1) & (row < count) & (lane == 13) & at_end
        next_first = next_first + summed(only(found, table))
        at_end = jnp.logical_and(at_end, mine == count - 1)
        joint = CORR * table * pltpu.roll(pltpu.roll(table, 7, 0), 2, 1)
        message = summed(
            only((lane < 12) | ((row == 0) & (lane < 14)) | ((row == count - 1) & (lane == 14)), table)
            + only((lane == 8) & (row < count - 1), pltpu.roll(joint, 122, 1))
        )

    last_lane = lane[:1] == SEG - 1
    covariance_own = covariance_own + only(last_lane, CORR * up_own * pltpu.roll(next_first, 115 + SEG - 1, 1))
    three = jnp.where(row == 0, estimate_own, jnp.where(row == 1, spread_own, covariance_own))
    stats[...] = three[:3, :SEG]

    def lanes_from(at):
        return jnp.sum(only((lane[:1] >= at) & (lane[:1] < at + 4), message), axis=1, keepdims=True)

    weight_sum, weighted_sum, pair_sum = lanes_from(0), lanes_from(4), lanes_from(8)
    root = float(np.sqrt(SEG * total))
    pick = lax.broadcasted_iota(jnp.int32, (1, 2), 1)
    combined[...] = jnp.where(
        pick == 0, root * (weighted_sum / weight_sum), root * (jnp.sqrt(weight_sum + 2.0 * pair_sum) / weight_sum)
    )

    for axis, count, mine in ((0, 2 * ny, slot_y), (1, nz, cz), (2, nx, cx)):
        for d in range(1, count):
            row_copy(axis, mine, lax.rem(mine + d, count)).wait_send()

    for end in range(2):

        @pl.when(jnp.logical_not(edges[1 - end]))
        def _(end=end):
            for p in range(2):
                half_copy(end, p).wait_send()

    power_copy.wait_send()
    for s in range(SEG):
        out_copy(s).wait()
    for s in range(-1, SEG):
        for pair in range(2):
            x_copy(s, pair).wait_send()


def writer(csd_in, stats_in, combined_in, csd, stats, combined, csd_v, stats_v, combined_v, sems):
    parts = [(csd_in.at[s], csd_v.at[s], csd.at[s]) for s in range(SEG)]
    parts += [(stats_in, stats_v, stats), (combined_in, combined_v, combined)]
    reads = [pltpu.make_async_copy(src, held, sems.at[0, i]) for i, (src, held, _) in enumerate(parts)]
    writes = [pltpu.make_async_copy(held, dst, sems.at[1, i]) for i, (_, held, dst) in enumerate(parts)]
    for read in reads:
        read.start()
    for read, write in zip(reads, writes):
        read.wait()
        write.start()
    for write in writes:
        write.wait()


def on_device(dims, strain, final_half, intersection_function, notch_mask, quality_flags):
    window, ones, twist, twos = tables()
    any_space = pl.BlockSpec(memory_space=pl.ANY)
    hbm = pl.BlockSpec(memory_space=pltpu.HBM)
    vmem = pl.BlockSpec(memory_space=pltpu.VMEM)
    dma = pltpu.SemaphoreType.DMA
    csd, stats, combined = pl.pallas_call(
        functools.partial(kernel, dims),
        out_shape=(
            jax.ShapeDtypeStruct((SEG, 128, 128), F32),
            jax.ShapeDtypeStruct((3, SEG), F32),
            jax.ShapeDtypeStruct((1, 2), F32),
        ),
        in_specs=[hbm] * 9,
        out_specs=(any_space, vmem, vmem),
        scratch_shapes=[
            pltpu.VMEM((SEG + 2, HALF, COLS), F32),
            pltpu.VMEM((HALF, COLS), F32),
            pltpu.VMEM((4 * ROWS, KPAD), BF16),
            pltpu.VMEM((2, ROWS, COLS), F32),
            pltpu.VMEM((4, 2, 256, 256), BF16),
            pltpu.VMEM((64, 128), F32),
            pltpu.VMEM((64, 128), jnp.int32),
            pltpu.VMEM((2, 2, KPAD, COLS), BF16),
            pltpu.VMEM((3, 2 * ROWS, COLS), F32),
            pltpu.VMEM((4, 2 * ROWS, 256), BF16),
            pltpu.VMEM((SEG + 1, 2, 4, ROWS, 128), F32),
            pltpu.VMEM((SEG + 1, 4, ROWS, 128), F32),
            pltpu.VMEM((SEG + 1, 2, 64, 128), F32),
            pltpu.VMEM((2, 64, 128), F32),
            pltpu.VMEM((SEG, 128, 128), F32),
            pltpu.VMEM((8, 128), F32),
            pltpu.VMEM((3, 16, 1, 128), F32),
            pltpu.VMEM((128, 128), F32),
            pltpu.VMEM((SEG, 64, 128), F32),
            pltpu.SMEM((SEG,), jnp.int32),
            dma((20,)),
            dma((2, 2)),
            dma((2, 2)),
            dma((SEG + 1, 2)),
            dma((SEG + 1, 2)),
            dma((2,)),
            dma((3, 16)),
            dma((3, 16)),
            dma((SEG + 1,)),
            pltpu.SemaphoreType.REGULAR,
            pltpu.SemaphoreType.REGULAR,
            pltpu.SemaphoreType.REGULAR,
        ],
        compiler_params=pltpu.CompilerParams(
            collective_id=0, has_side_effects=True, vmem_limit_bytes=67_043_328
        ),
    )(
        strain,
        final_half,
        intersection_function.reshape(64, 128),
        notch_mask.reshape(64, 128),
        quality_flags,
        window,
        ones,
        twist,
        twos,
    )
    csd, stats, combined = pl.pallas_call(
        writer,
        out_shape=(
            jax.ShapeDtypeStruct((SEG, 128, 128), F32),
            jax.ShapeDtypeStruct((3, SEG), F32),
            jax.ShapeDtypeStruct((1, 2), F32),
        ),
        in_specs=[any_space] * 3,
        out_specs=[any_space] * 3,
        scratch_shapes=[
            pltpu.VMEM((SEG, 128, 128), F32),
            pltpu.VMEM((3, SEG), F32),
            pltpu.VMEM((1, 2), F32),
            dma((2, SEG + 2)),
        ],
    )(csd, stats, combined)
    csd = csd.reshape(SEG, 64, 2, 128).transpose(0, 2, 1, 3).reshape(SEG, 2, 64 * 128)
    return csd, stats, combined.reshape(2)


def solution(mesh):
    count = mesh.shape["tm"]
    dims = (4, 8, 8) if count == 256 else (2, 2, count // 4)
    return jax.shard_map(
        functools.partial(on_device, dims),
        mesh=mesh,
        in_specs=(P("det", "tm", None, None), P("det", None, None), P("det"), P("det"), P("tm")),
        out_specs=(P("tm", None, "det"), P(None, "tm"), P()),
        check_vma=False,
    )
```
